16 devices in a mesh: dp: 1, sp: 16 (over x, y, z, core).
Axes of the slice: x: 2, y: 2, z: 2, core: 2. Of those that a mesh axis runs over, the one named last changes fastest.
Arguments:
- x: bfloat16 [4096, 3072], P(('dp', 'sp'))
- gain: bfloat16 [3072], replicated
- wq: bfloat16 [3072, 3072], replicated
- wk: bfloat16 [3072, 1024], replicated
- wv: bfloat16 [3072, 1024], replicated
- wo: bfloat16 [3072, 3072], replicated
Outputs:
- output: bfloat16 [4096, 3072], P(('dp', 'sp'))
All inputs are finite; a program needn't handle non-finite values.
Results may differ from the reference program's by a relative error of at most 0.012.
Values are sent between devices in bfloat16 or wider.
A program may use at most 2 GiB of HBM per device.

```python
import jax
import jax.numpy as jnp
from jax import lax

ROWS = 4096
D = 3072
HEADS = 24
KV_HEADS = 8
HEAD = 128
THETA = 10000


def setup_inputs(seed: int = 0, part: int = 0) -> dict:
    kx, kn, kq, kk, kv, ko = jax.random.split(jax.random.key(seed), 6)

    def weights(key, rows, columns):
        return jax.random.normal(key, (rows, columns), jnp.float32) * rows**-0.5

    drawn = {
        "x": jax.random.normal(jax.random.fold_in(kx, part), (ROWS, D), jnp.float32),
        "gain": 1 + 0.1 * jax.random.normal(kn, (D,), jnp.float32),
        "wq": 2 * weights(kq, D, HEADS * HEAD),
        "wk": 2 * weights(kk, D, KV_HEADS * HEAD),
        "wv": 4 * weights(kv, D, KV_HEADS * HEAD),
        "wo": weights(ko, HEADS * HEAD, D),
    }
    return {k: v.astype(jnp.bfloat16) for k, v in drawn.items()}


def normed(x, gain):
    wide = x.astype(jnp.float32)
    scale = lax.rsqrt(jnp.mean(wide * wide, -1, keepdims=True) + 1e-6)
    return (wide * scale * gain.astype(jnp.float32)).astype(jnp.bfloat16)


def turned(t, place, theta):
    half = t.shape[-1] // 2
    angle = place.astype(jnp.float32)[:, None] * theta ** (-jnp.arange(half, dtype=jnp.float32) / half)
    cos, sin = jnp.cos(angle)[:, None], jnp.sin(angle)[:, None]
    a, b = t[..., :half].astype(jnp.float32), t[..., half:].astype(jnp.float32)
    return jnp.concatenate([a * cos - b * sin, b * cos + a * sin], -1).astype(jnp.bfloat16)


def matmul(a, w):
    return jnp.dot(a, w, preferred_element_type=jnp.float32).astype(jnp.bfloat16)


def einsum(form, a, b):
    return jnp.einsum(form, a.astype(jnp.float32), b.astype(jnp.float32))


def attention(q, k, v):
    scores = einsum("tgsd,ugd->gstu", q, k) * q.shape[-1] ** -0.5
    token = jnp.arange(q.shape[0])
    scores = jnp.where(token[:, None] >= token, scores, -jnp.inf)
    weights = jax.nn.softmax(scores, -1).astype(jnp.bfloat16)
    return einsum("gstu,ugd->tgsd", weights, v).astype(jnp.bfloat16)


def reference(x, gain, wq, wk, wv, wo):
    a, place = normed(x, gain), jnp.arange(ROWS)
    q = turned(matmul(a, wq).reshape(ROWS, HEADS, HEAD), place, THETA).reshape(ROWS, KV_HEADS, -1, HEAD)
    k = turned(matmul(a, wk).reshape(ROWS, KV_HEADS, HEAD), place, THETA)
    v = matmul(a, wv).reshape(ROWS, KV_HEADS, HEAD)
    seen = attention(q, k, v).reshape(ROWS, HEADS * HEAD)
    return (x.astype(jnp.float32) + jnp.dot(seen, wo, preferred_element_type=jnp.float32)).astype(jnp.bfloat16)
```

```python
import functools

import jax
import jax.numpy as jnp
import numpy as np
from jax import lax
from jax.experimental import pallas as pl
from jax.experimental.pallas import tpu as pltpu
from jax.sharding import PartitionSpec as P

HEAD = 128
HALF = HEAD // 2
THETA = 10000
CHIPS = 8
GROUP = 3
ROWS = 256
D = 3072
HIDDEN = -2e30
E = HEAD**-0.5 * 1.4426950408889634
OUT = (6, 1, 5, 2, 3, 4, 7, 0)
IN = (0, 6, 1, 5, 2, 3, 4, 7)
SLOTS = 4
KV_TILES, Q_TILES = CHIPS, CHIPS * GROUP // 2
TILES = KV_TILES + Q_TILES
COLS = 256
F32, BF16 = jnp.float32, jnp.bfloat16


def _dot(a, b, ca, cb):
    return lax.dot_general(a, b, (((ca,), (cb,)), ((), ())), preferred_element_type=F32)


def _pick(i, table):
    r = jnp.int32(table[0])
    for n, v in enumerate(table[1:], 1):
        r = jnp.where(i == n, jnp.int32(v), r)
    return r


def _kernel(x_hbm, gain_ref, rot_ref, off_ref, wq, wk, wv, wo, y_ref, xs, a, cos_s, sin_s, wt, wos, kv_out, kv, q_out, qs, o_out, os, part, tops, yacc,
            x_sem, w_sem, wo_sem, kv_ss, kv_rs, rl_ss, q_ss, q_rs, o_ss, o_rs):
    me = lax.axis_index("sp")
    chip, core = me // 2, me % 2
    sibling = 2 * chip + 1 - core

    def other(mask):
        return jnp.bitwise_xor(chip, mask)

    def remote(src, dst, ss, rs, dev):
        return pltpu.make_async_remote_copy(src_ref=src, dst_ref=dst, send_sem=ss, recv_sem=rs, device_id={"sp": dev}, device_id_type=pl.DeviceIdType.MESH)

    x_copy = pltpu.make_async_copy(x_hbm, xs, x_sem)
    x_copy.start()

    def tile_copies(t, slot):
        def halves(w0, at0, w1, at1):
            at0, at1 = pl.multiple_of(at0 * HEAD, HEAD), pl.multiple_of(at1 * HEAD, HEAD)
            return [pltpu.make_async_copy(w0.at[:, pl.ds(at0, HEAD)], wt.at[slot, :, pl.ds(0, HEAD)], w_sem.at[slot, 0]),
                    pltpu.make_async_copy(w1.at[:, pl.ds(at1, HEAD)], wt.at[slot, :, pl.ds(HEAD, HEAD)], w_sem.at[slot, 1])]
        d = other(_pick(t, OUT))
        j = t - KV_TILES
        h, pair = j // 4, j % 4
        d0, d1 = other(_pick(2 * pair, OUT)), other(_pick(2 * pair + 1, OUT))
        return halves(wk, d, wv, d), halves(wq, GROUP * d0 + h, wq, GROUP * d1 + h)

    def start_tile(t):
        keys, queries = tile_copies(t, t % SLOTS)

        @pl.when(t < KV_TILES)
        def _():
            for c in keys:
                c.start()

        @pl.when((t >= KV_TILES) & (t < TILES))
        def _():
            for c in queries:
                c.start()

    def wait_tile(t):
        for c in tile_copies(jnp.int32(0), t % SLOTS)[0]:
            c.wait()

    for t in range(SLOTS - 1):
        start_tile(jnp.int32(t))

    barrier = pltpu.get_barrier_semaphore()
    for m in range(1, CHIPS):
        pl.semaphore_signal(barrier, inc=1, device_id={"sp": 2 * other(m) + core}, device_id_type=pl.DeviceIdType.MESH)
    pl.semaphore_signal(barrier, inc=1, device_id={"sp": sibling}, device_id_type=pl.DeviceIdType.MESH)

    c0, s0 = off_ref[0, pl.ds(me, 1), :], off_ref[1, pl.ds(me, 1), :]
    cos_s[...] = c0 * rot_ref[0] - s0 * rot_ref[1]
    sin = s0 * rot_ref[0] + c0 * rot_ref[1]
    sin_s[...] = jnp.where(lax.broadcasted_iota(jnp.int32, sin.shape, 1) < HALF, -sin, sin)

    x_copy.wait()

    def norm(i, _):
        rows = pl.ds(pl.multiple_of(i * 16, 16), 16)
        wide = xs[rows, :].astype(F32)
        scale = lax.rsqrt(jnp.mean(wide * wide, -1, keepdims=True) + 1e-6)
        a[rows, :] = (wide * scale * gain_ref[...].astype(F32)).astype(BF16)
        return _

    lax.fori_loop(0, ROWS // 16, norm, None)
    pl.semaphore_wait(barrier, CHIPS)

    def turned(t):
        t = t.astype(BF16).astype(F32)
        return (t * cos_s[...] + pltpu.roll(t, HALF, 1) * sin_s[...]).astype(BF16)

    def project(t):
        wait_tile(t)
        start_tile(t + SLOTS - 1)
        return _dot(a[...], wt[t % SLOTS], 1, 0)

    def kv_copy(i):
        return remote(kv_out.at[i], kv.at[me], kv_ss.at[i], kv_rs.at[me], 2 * other(_pick(i, OUT)) + core)

    def project_kv(i, _):
        r = project(i)
        k, v = turned(r[:, :HEAD]), r[:, HEAD:].astype(BF16).T

        def put(ref, n):
            ref[n, :ROWS, :] = k
            ref[n, ROWS : ROWS + HEAD, :] = v[:, :HEAD]
            ref[n, ROWS + HEAD :, :] = v[:, HEAD:]

        @pl.when(i < CHIPS - 1)
        def _():
            put(kv_out, i)
            kv_copy(i).start()

        @pl.when(i == CHIPS - 1)
        def _():
            put(kv, me)

        return _

    lax.fori_loop(0, KV_TILES, project_kv, None)

    def q_copy(h, i):
        return remote(q_out.at[h, i], qs.at[h, chip], q_ss.at[h, i], q_rs.at[h, chip], 2 * other(_pick(i, OUT)) + core)

    def project_q(j, _):
        r = project(j + KV_TILES)
        h, i = j // 4, 2 * (j % 4)
        q0, q1 = turned(r[:, :HEAD]), turned(r[:, HEAD:])
        q_out[h, i] = q0
        q_copy(h, i).start()

        @pl.when(i + 1 < CHIPS - 1)
        def _():
            q_out[h, i + 1] = q1
            q_copy(h, i + 1).start()

        @pl.when(i + 1 == CHIPS - 1)
        def _():
            qs[h, chip] = q1

        return _

    lax.fori_loop(0, Q_TILES, project_q, None)

    def wo_copy(h, g):
        return pltpu.make_async_copy(wo.at[pl.ds((GROUP * g + h) * HEAD, HEAD), :], wos.at[h, pl.ds(g * HEAD, HEAD), :], wo_sem.at[h, g])

    for h in range(GROUP):
        for g in range(CHIPS):
            wo_copy(h, g).start()

    def relay(s):
        b = 2 * s + core
        return remote(kv.at[b], kv.at[b], rl_ss.at[s], kv_rs.at[b], sibling)

    def arrive(h, p):
        s = other(_pick(p, IN))

        @pl.when(h == 0)
        def _():
            @pl.when(p > 0)
            def _():
                b = 2 * s + core
                remote(kv_out.at[0], kv.at[b], kv_ss.at[0], kv_rs.at[b], sibling).wait_recv()

            relay(s).start()
            b = 2 * s + 1 - core
            remote(kv_out.at[0], kv.at[b], kv_ss.at[0], kv_rs.at[b], sibling).wait_recv()

        @pl.when(p > 0)
        def _():
            remote(q_out.at[0, 0], qs.at[h, s], q_ss.at[0, 0], q_rs.at[h, s], sibling).wait_recv()

    ones = jnp.ones((8, 2 * ROWS), BF16)

    def attend(h, items):
        scores = []
        for sq, sk, masked in items:
            k = jnp.concatenate([kv[2 * sk, :ROWS, :], kv[2 * sk + 1, :ROWS, :]], axis=0)
            s = _dot(k, qs[h, sq], 1, 1)
            if masked:
                gap = lax.broadcasted_iota(jnp.int32, s.shape, 1) - lax.broadcasted_iota(jnp.int32, s.shape, 0)
                s = jnp.where(gap >= -ROWS * core, s, HIDDEN)
            scores.append(s)
        weights = []
        for (sq, sk, _), s in zip(items, scores):
            top = s.max(axis=0, keepdims=True)
            tops[sq * CHIPS + sk] = jnp.broadcast_to(top, (8, ROWS))
            weights.append(jnp.exp2((s - top) * E).astype(BF16))
        for (sq, sk, _), p in zip(items, weights):
            v = jnp.concatenate([kv[2 * sk + c, ROWS + n * HEAD : ROWS + (n + 1) * HEAD, :] for c in range(2) for n in range(2)], axis=1)
            part[sq * CHIPS + sk] = _dot(jnp.concatenate([v, ones], axis=0), p, 1, 0)

    def o_copy(h, i):
        return remote(o_out.at[h, i], os.at[h, chip], o_ss.at[h, i], o_rs.at[h, chip], 2 * other(_pick(i, OUT)) + core)

    def head(h, _):
        def two(n, _):
            arrive(h, 2 * n)
            arrive(h, 2 * n + 1)
            s0, s1 = other(_pick(2 * n, IN)), other(_pick(2 * n + 1, IN))
            attend(h, [(s0, s0, True), (s1, s1, True), (jnp.maximum(s0, s1), jnp.minimum(s0, s1), False)])

            def earlier(m, _):
                s2 = other(_pick(m, IN))
                attend(h, [(jnp.maximum(s0, s2), jnp.minimum(s0, s2), False), (jnp.maximum(s1, s2), jnp.minimum(s1, s2), False)])
                return _

            lax.fori_loop(0, 2 * n, earlier, None)
            return _

        lax.fori_loop(0, CHIPS // 2, two, None)

        def finish(i, _):
            sq = other(_pick(i, OUT))
            top = lax.fori_loop(0, sq + 1, lambda n, t: jnp.maximum(t, tops[sq * CHIPS + n]), jnp.full((8, ROWS), HIDDEN, F32))

            def add(n, acc):
                keep = jnp.exp2((tops[sq * CHIPS + n] - top) * E)
                return acc + part[sq * CHIPS + n] * keep[:1]

            acc = lax.fori_loop(0, sq + 1, add, jnp.zeros((HEAD + 8, ROWS), F32))
            o = (acc[:HEAD] * (1 / acc[HEAD : HEAD + 1])).T.astype(BF16)

            @pl.when(i < CHIPS - 1)
            def _():
                o_out[h, i] = o
                o_copy(h, i).start()

            @pl.when(i == CHIPS - 1)
            def _():
                os[h, chip] = o

            return _

        lax.fori_loop(0, CHIPS, finish, None)
        return _

    lax.fori_loop(0, GROUP, head, None)

    for h in range(GROUP):
        for g in range(CHIPS):
            wo_copy(h, g).wait()
        for m in OUT[:-1]:
            remote(o_out.at[0, 0], os.at[h, other(m)], o_ss.at[0, 0], o_rs.at[h, other(m)], sibling).wait_recv()

        def columns(n, _):
            at = pl.ds(pl.multiple_of(n * COLS, COLS), COLS)
            seen = jnp.concatenate([os[h, g] for g in range(CHIPS)], axis=1)
            r = _dot(seen, wos[h, :, at], 1, 0)
            if h > 0:
                r += yacc[:, at]
            if h < GROUP - 1:
                yacc[:, at] = r
            else:
                y_ref[:, at] = (xs[:, at].astype(F32) + r).astype(BF16)
            return _

        lax.fori_loop(0, D // COLS, columns, None)

    for s in range(CHIPS):
        relay(s).wait_send()
    for i in range(CHIPS - 1):
        kv_copy(i).wait_send()
        for h in range(GROUP):
            q_copy(h, i).wait_send()
            o_copy(h, i).wait_send()


def _tables():
    rate = float(THETA) ** (-np.arange(HALF) / HALF)
    def both(place):
        angle = np.tile(place[:, None] * rate, 2)
        return np.stack([np.cos(angle), np.sin(angle)]).astype(np.float32)
    return both(np.arange(ROWS, dtype=np.float64)), both(ROWS * np.arange(2 * CHIPS, dtype=np.float64))


def solution(mesh):
    rot, off = _tables()
    dma = pltpu.SemaphoreType.DMA
    anywhere, vmem = pl.BlockSpec(memory_space=pl.ANY), pl.BlockSpec(memory_space=pltpu.VMEM)

    def step(x, gain, wq, wk, wv, wo):
        block = (ROWS, HEAD)
        return pl.pallas_call(
            _kernel,
            out_shape=jax.ShapeDtypeStruct((ROWS, D), BF16),
            in_specs=[anywhere, vmem, vmem, vmem, anywhere, anywhere, anywhere, anywhere],
            out_specs=vmem,
            scratch_shapes=[
                pltpu.VMEM((ROWS, D), BF16),
                pltpu.VMEM((ROWS, D), BF16),
                pltpu.VMEM(block, F32),
                pltpu.VMEM(block, F32),
                pltpu.VMEM((SLOTS, D, 2 * HEAD), BF16),
                pltpu.VMEM((GROUP, CHIPS * HEAD, D), BF16),
                pltpu.VMEM((CHIPS - 1, 2 * ROWS, HEAD), BF16),
                pltpu.VMEM((2 * CHIPS, 2 * ROWS, HEAD), BF16),
                pltpu.VMEM((GROUP, CHIPS - 1, *block), BF16),
                pltpu.VMEM((GROUP, CHIPS, *block), BF16),
                pltpu.VMEM((GROUP, CHIPS - 1, *block), BF16),
                pltpu.VMEM((GROUP, CHIPS, *block), BF16),
                pltpu.VMEM((CHIPS * CHIPS, HEAD + 8, ROWS), F32),
                pltpu.VMEM((CHIPS * CHIPS, 8, ROWS), F32),
                pltpu.VMEM((ROWS, D), F32),
                dma,
                dma((SLOTS, 2)),
                dma((GROUP, CHIPS)),
                dma((CHIPS,)),
                dma((2 * CHIPS,)),
                dma((CHIPS,)),
                dma((GROUP, CHIPS)),
                dma((GROUP, CHIPS)),
                dma((GROUP, CHIPS)),
                dma((GROUP, CHIPS)),
            ],
            compiler_params=pltpu.CompilerParams(collective_id=0, has_side_effects=True, vmem_limit_bytes=67043328),
        )(x, gain.reshape(1, D), jnp.asarray(rot), jnp.asarray(off), wq, wk, wv, wo)

    tokens, whole = P(("dp", "sp"), None), P(None, None)
    return jax.shard_map(
        step,
        mesh=mesh,
        in_specs=(tokens, P(None), whole, whole, whole, whole),
        out_specs=tokens,
        check_vma=False,
    )
```

```python
import functools

import jax
import jax.numpy as jnp
import numpy as np
from jax import lax
from jax.experimental import pallas as pl
from jax.experimental.pallas import tpu as pltpu
from jax.sharding import PartitionSpec as P

HEAD = 128
HALF = HEAD // 2
THETA = 10000
CHIPS = 8
GROUP = 3
ROWS = 256
D = 3072
HIDDEN = -2e30
E = HEAD**-0.5 * 1.4426950408889634
OUT = (6, 1, 5, 2, 3, 4, 7, 0)
IN = (0, 6, 1, 5, 2, 3, 4, 7)
SLOTS = 6
KV_TILES, Q_TILES = CHIPS, CHIPS * GROUP // 2
TILES = KV_TILES + Q_TILES
COLS = 512
X_PARTS = 4
F32, BF16 = jnp.float32, jnp.bfloat16


def _dot(a, b, ca, cb):
    return lax.dot_general(a, b, (((ca,), (cb,)), ((), ())), preferred_element_type=F32)


def _pick(i, table):
    r = jnp.int32(table[0])
    for n, v in enumerate(table[1:], 1):
        r = jnp.where(i == n, jnp.int32(v), r)
    return r


def _kernel(x_hbm, gain_ref, rot_ref, off_ref, wq, wk, wv, wo, y_ref, xs, a, cos_s, sin_s, wt, wos, kv_out, kv, q_out, qs, o_out, os, part, tops, yacc,
            x_sem, own_sem, ownq_sem, w_sem, wo_sem, kv_ss, kv_rs, rl_ss, q_ss, q_rs, o_ss, o_rs):
    me = lax.axis_index("sp")
    chip, core = me // 2, me % 2
    sibling = 2 * chip + 1 - core

    def other(mask):
        return jnp.bitwise_xor(chip, mask)

    def remote(src, dst, ss, rs, dev):
        return pltpu.make_async_remote_copy(src_ref=src, dst_ref=dst, send_sem=ss, recv_sem=rs, device_id={"sp": dev}, device_id_type=pl.DeviceIdType.MESH)

    def x_copy(i):
        rows = pl.ds(pl.multiple_of(i * (ROWS // X_PARTS), ROWS // X_PARTS), ROWS // X_PARTS)
        return pltpu.make_async_copy(x_hbm.at[rows], xs.at[rows], x_sem.at[i])

    for i in range(X_PARTS):
        x_copy(i).start()

    def tile_copies(t, slot):
        def halves(w0, at0, w1, at1):
            at0, at1 = pl.multiple_of(at0 * HEAD, HEAD), pl.multiple_of(at1 * HEAD, HEAD)
            return [pltpu.make_async_copy(w0.at[:, pl.ds(at0, HEAD)], wt.at[slot, :, pl.ds(0, HEAD)], w_sem.at[slot, 0]),
                    pltpu.make_async_copy(w1.at[:, pl.ds(at1, HEAD)], wt.at[slot, :, pl.ds(HEAD, HEAD)], w_sem.at[slot, 1])]
        d = other(_pick(t, OUT))
        j = t - KV_TILES
        h, pair = j // 4, j % 4
        d0, d1 = other(_pick(2 * pair, OUT)), other(_pick(2 * pair + 1, OUT))
        return halves(wk, d, wv, d), halves(wq, GROUP * d0 + h, wq, GROUP * d1 + h)

    def start_tile(t):
        keys, queries = tile_copies(t, t % SLOTS)

        @pl.when(t < KV_TILES)
        def _():
            for c in keys:
                c.start()

        @pl.when((t >= KV_TILES) & (t < TILES))
        def _():
            for c in queries:
                c.start()

    def wait_tile(t):
        for c in tile_copies(jnp.int32(0), t % SLOTS)[0]:
            c.wait()

    for t in range(SLOTS):
        start_tile(jnp.int32(t))

    barrier = pltpu.get_barrier_semaphore()
    for m in range(1, CHIPS):
        pl.semaphore_signal(barrier, inc=1, device_id={"sp": 2 * other(m) + core}, device_id_type=pl.DeviceIdType.MESH)
    pl.semaphore_signal(barrier, inc=1, device_id={"sp": sibling}, device_id_type=pl.DeviceIdType.MESH)

    c0, s0 = off_ref[0, pl.ds(me, 1), :], off_ref[1, pl.ds(me, 1), :]
    cos_s[...] = c0 * rot_ref[0] - s0 * rot_ref[1]
    sin = s0 * rot_ref[0] + c0 * rot_ref[1]
    sin_s[...] = jnp.where(lax.broadcasted_iota(jnp.int32, sin.shape, 1) < HALF, -sin, sin)

    gain = gain_ref[...].reshape(1, D).astype(F32)

    def norm(i, _):
        x_copy(i).wait()
        rows = pl.ds(pl.multiple_of(i * (ROWS // X_PARTS), ROWS // X_PARTS), ROWS // X_PARTS)
        wide = xs[rows, :].astype(F32)
        scale = lax.rsqrt(jnp.mean(wide * wide, -1, keepdims=True) + 1e-6)
        a[rows, :] = (wide * scale * gain).astype(BF16)
        return _

    with jax.named_scope("norm"):
        lax.fori_loop(0, X_PARTS, norm, None)
    with jax.named_scope("barrier"):
        pl.semaphore_wait(barrier, CHIPS)

    def turned(t):
        t = t.astype(BF16).astype(F32)
        return (t * cos_s[...] + pltpu.roll(t, HALF, 1) * sin_s[...]).astype(BF16)

    def project(t):
        for n in range(2):
            wait_tile(t + n)
        return [_dot(a[...], wt[(t + n) % SLOTS], 1, 0) for n in range(2)]

    def refill(t):
        for n in range(2):
            start_tile(t + n + SLOTS)

    def kv_copy(i):
        return remote(kv_out.at[i], kv.at[me], kv_ss.at[i], kv_rs.at[me], 2 * other(_pick(i, OUT)) + core)

    def project_kv(n, _):
        rs = project(2 * n)
        for i, r in zip((2 * n, 2 * n + 1), rs):
            k, v = turned(r[:, :HEAD]), r[:, HEAD:].astype(BF16).T
            kv_out[i, :ROWS, :] = k
            kv_out[i, ROWS : ROWS + HEAD, :] = v[:, :HEAD]
            kv_out[i, ROWS + HEAD :, :] = v[:, HEAD:]
        refill(2 * n)
        kv_copy(2 * n).start()

        @pl.when(n < KV_TILES // 2 - 1)
        def _():
            kv_copy(2 * n + 1).start()

        return _

    with jax.named_scope("project_kv"):
        lax.fori_loop(0, KV_TILES // 2, project_kv, None)
    own_kv = pltpu.make_async_copy(kv_out.at[CHIPS - 1], kv.at[me], own_sem)
    own_kv.start()

    def relay(s):
        b = 2 * s + core
        return remote(kv.at[b], kv.at[b], rl_ss.at[s], kv_rs.at[b], sibling)

    def pass_on(p):
        s = other(_pick(p, OUT))
        b = 2 * s + core
        remote(kv_out.at[0], kv.at[b], kv_ss.at[0], kv_rs.at[b], sibling).wait_recv()
        relay(s).start()

    def q_copy(h, i):
        return remote(q_out.at[h, i], qs.at[h, chip], q_ss.at[h, i], q_rs.at[h, chip], 2 * other(_pick(i, OUT)) + core)

    def project_q(n, _):
        rs = project(2 * n + KV_TILES)
        h, i0 = n // 2, 4 * (n % 2)
        for m, r in enumerate(rs):
            q_out[h, i0 + 2 * m] = turned(r[:, :HEAD])
            q_out[h, i0 + 2 * m + 1] = turned(r[:, HEAD:])
        refill(2 * n + KV_TILES)
        for m in range(3):
            q_copy(h, i0 + m).start()

        @pl.when(n % 2 == 0)
        def _():
            q_copy(h, i0 + 3).start()

        @pl.when(n > 0)
        def _():
            pass_on(n - 1)

        return _

    with jax.named_scope("project_q"):
        own_kv.wait()
        relay(chip).start()
        lax.fori_loop(0, Q_TILES // 2, project_q, None)
        pass_on(jnp.int32(5))
        pass_on(jnp.int32(6))
        own_q = [pltpu.make_async_copy(q_out.at[h, CHIPS - 1], qs.at[h, chip], ownq_sem.at[h]) for h in range(GROUP)]
        for c in own_q:
            c.start()
        for c in own_q:
            c.wait()

    def wo_copy(h, g):
        return pltpu.make_async_copy(wo.at[pl.ds((GROUP * g + h) * HEAD, HEAD), :], wos.at[h, pl.ds(g * HEAD, HEAD), :], wo_sem.at[h, g])

    for h in range(GROUP):
        for g in range(CHIPS):
            wo_copy(h, g).start()

    def arrive(h, p):
        s = other(_pick(p, IN))

        @pl.when(h == 0)
        def _():
            b = 2 * s + 1 - core
            remote(kv_out.at[0], kv.at[b], kv_ss.at[0], kv_rs.at[b], sibling).wait_recv()

        @pl.when(p > 0)
        def _():
            remote(q_out.at[0, 0], qs.at[h, s], q_ss.at[0, 0], q_rs.at[h, s], sibling).wait_recv()

    def at(sq, sk):
        return sq * (sq + 1) // 2 + sk

    ones = jnp.ones((8, 2 * ROWS), BF16)

    def attend(h, items):
        scores = []
        for sq, sk, masked in items:
            k = jnp.concatenate([kv[2 * sk, :ROWS, :], kv[2 * sk + 1, :ROWS, :]], axis=0)
            s = _dot(k, qs[h, sq], 1, 1)
            if masked:
                gap = lax.broadcasted_iota(jnp.int32, s.shape, 1) - lax.broadcasted_iota(jnp.int32, s.shape, 0)
                s = jnp.where(gap >= -ROWS * core, s, HIDDEN)
            scores.append(s)
        weights = []
        for (sq, sk, _), s in zip(items, scores):
            top = s.max(axis=0, keepdims=True)
            tops[at(sq, sk)] = jnp.broadcast_to(top, (8, ROWS))
            weights.append(jnp.exp2((s - top) * E).astype(BF16))
        for (sq, sk, _), p in zip(items, weights):
            v = jnp.concatenate([kv[2 * sk + c, ROWS + n * HEAD : ROWS + (n + 1) * HEAD, :] for c in range(2) for n in range(2)], axis=1)
            part[at(sq, sk)] = _dot(jnp.concatenate([v, ones], axis=0), p, 1, 0)

    def o_copy(h, i):
        sq = other(_pick(i, OUT))
        return remote(o_out.at[h, sq], os.at[h, chip], o_ss.at[h, i], o_rs.at[h, chip], 2 * sq + core)

    def head(h, _):
        def two(n, _):
            with jax.named_scope("arrive"):
                arrive(h, 2 * n)
                arrive(h, 2 * n + 1)
            s0, s1 = other(_pick(2 * n, IN)), other(_pick(2 * n + 1, IN))
            attend(h, [(s0, s0, True), (s1, s1, True), (jnp.maximum(s0, s1), jnp.minimum(s0, s1), False)])

            def earlier(m, _):
                s2, s3 = other(_pick(2 * m, IN)), other(_pick(2 * m + 1, IN))
                attend(h, [(jnp.maximum(a, b), jnp.minimum(a, b), False) for b in (s2, s3) for a in (s0, s1)])
                return _

            with jax.named_scope("earlier"):
                lax.fori_loop(0, n, earlier, None)
            return _

        with jax.named_scope("attend"):
            lax.fori_loop(0, CHIPS // 2, two, None)

        def finish(sq):
            top = functools.reduce(jnp.maximum, [tops[at(sq, n)] for n in range(sq + 1)])
            acc = sum(part[at(sq, n)] * jnp.exp2((tops[at(sq, n)] - top) * E)[:1] for n in range(sq + 1))
            o_out[h, sq] = (acc[:HEAD] * (1 / acc[HEAD : HEAD + 1])).T.astype(BF16)

        def give(i, _):
            o_copy(h, i).start()
            return _

        with jax.named_scope("finish"):
            for sq in range(CHIPS):
                finish(sq)
            lax.fori_loop(0, CHIPS - 1, give, None)
        return _

    with jax.named_scope("heads"):
        lax.fori_loop(0, GROUP, head, None)

    def results(h):
        with jax.named_scope("wo_wait"):
            for g in range(CHIPS):
                wo_copy(h, g).wait()
        with jax.named_scope("o_wait"):
            for m in OUT[:-1]:
                remote(o_out.at[0, 0], os.at[h, other(m)], o_ss.at[0, 0], o_rs.at[h, other(m)], sibling).wait_recv()

    def columns(heads, last):
        def body(n, _):
            cols = pl.ds(pl.multiple_of(n * COLS, COLS), COLS)
            seen = jnp.concatenate([os[h, g] for h in heads for g in range(CHIPS)], axis=1)
            w = jnp.concatenate([wos[h, :, cols] for h in heads], axis=0)
            r = _dot(seen, w, 1, 0)
            if last:
                y_ref[:, cols] = (xs[:, cols].astype(F32) + (yacc[:, cols] + r)).astype(BF16)
            else:
                yacc[:, cols] = r
            return _

        with jax.named_scope("columns"):
            lax.fori_loop(0, D // COLS, body, None)

    own_o = [pltpu.make_async_copy(o_out.at[h, chip], os.at[h, chip], ownq_sem.at[h]) for h in range(GROUP)]
    for c in own_o:
        c.start()
    for c in own_o:
        c.wait()
    results(0)
    results(1)
    columns((0, 1), False)
    results(2)
    columns((2,), True)

    with jax.named_scope("sent"):
        for s in range(CHIPS):
            relay(s).wait_send()
        for i in range(CHIPS - 1):
            kv_copy(i).wait_send()
            for h in range(GROUP):
                q_copy(h, i).wait_send()
                o_copy(h, i).wait_send()


def _tables():
    rate = float(THETA) ** (-np.arange(HALF) / HALF)
    def both(place):
        angle = np.tile(place[:, None] * rate, 2)
        return np.stack([np.cos(angle), np.sin(angle)]).astype(np.float32)
    return both(np.arange(ROWS, dtype=np.float64)), both(ROWS * np.arange(2 * CHIPS, dtype=np.float64))


def solution(mesh):
    rot, off = _tables()
    dma = pltpu.SemaphoreType.DMA
    anywhere, vmem = pl.BlockSpec(memory_space=pl.ANY), pl.BlockSpec(memory_space=pltpu.VMEM)

    def step(x, gain, wq, wk, wv, wo):
        block = (ROWS, HEAD)
        return pl.pallas_call(
            _kernel,
            out_shape=jax.ShapeDtypeStruct((ROWS, D), BF16),
            in_specs=[anywhere, vmem, vmem, vmem, anywhere, anywhere, anywhere, anywhere],
            out_specs=vmem,
            scratch_shapes=[
                pltpu.VMEM((ROWS, D), BF16),
                pltpu.VMEM((ROWS, D), BF16),
                pltpu.VMEM(block, F32),
                pltpu.VMEM(block, F32),
                pltpu.VMEM((SLOTS, D, 2 * HEAD), BF16),
                pltpu.VMEM((GROUP, CHIPS * HEAD, D), BF16),
                pltpu.VMEM((CHIPS, 2 * ROWS, HEAD), BF16),
                pltpu.VMEM((2 * CHIPS, 2 * ROWS, HEAD), BF16),
                pltpu.VMEM((GROUP, CHIPS, *block), BF16),
                pltpu.VMEM((GROUP, CHIPS, *block), BF16),
                pltpu.VMEM((GROUP, CHIPS, *block), BF16),
                pltpu.VMEM((GROUP, CHIPS, *block), BF16),
                pltpu.VMEM((CHIPS * (CHIPS + 1) // 2, HEAD + 8, ROWS), F32),
                pltpu.VMEM((CHIPS * (CHIPS + 1) // 2, 8, ROWS), F32),
                pltpu.VMEM((ROWS, D), F32),
                dma((X_PARTS,)),
                dma,
                dma((GROUP,)),
                dma((SLOTS, 2)),
                dma((GROUP, CHIPS)),
                dma((CHIPS,)),
                dma((2 * CHIPS,)),
                dma((CHIPS,)),
                dma((GROUP, CHIPS)),
                dma((GROUP, CHIPS)),
                dma((GROUP, CHIPS)),
                dma((GROUP, CHIPS)),
            ],
            compiler_params=pltpu.CompilerParams(collective_id=0, has_side_effects=True, vmem_limit_bytes=67043328),
        )(x, gain, jnp.asarray(rot), jnp.asarray(off), wq, wk, wv, wo)

    tokens, whole = P(("dp", "sp"), None), P(None, None)
    return jax.shard_map(
        step,
        mesh=mesh,
        in_specs=(tokens, P(None), whole, whole, whole, whole),
        out_specs=tokens,
        check_vma=False,
    )
```

```python
import functools

import jax
import jax.numpy as jnp
import numpy as np
from jax import lax
from jax.experimental import pallas as pl
from jax.experimental.pallas import tpu as pltpu
from jax.sharding import PartitionSpec as P

HEAD = 128
HALF = HEAD // 2
THETA = 10000
CHIPS = 8
GROUP = 3
ROWS = 256
D = 3072
HIDDEN = -2e30
E = HEAD**-0.5 * 1.4426950408889634
OUT = (6, 1, 5, 2, 3, 4, 7, 0)
IN = (0, 6, 1, 5, 2, 3, 4, 7)
SLOTS = 6
KV_TILES, Q_TILES = CHIPS, CHIPS * GROUP // 2
TILES = KV_TILES + Q_TILES
COLS = 512
X_PARTS = 4
STEP = 3
F32, BF16 = jnp.float32, jnp.bfloat16


def _dot(a, b, ca, cb):
    return lax.dot_general(a, b, (((ca,), (cb,)), ((), ())), preferred_element_type=F32)


def _pick(i, table):
    r = jnp.int32(table[0])
    for n, v in enumerate(table[1:], 1):
        r = jnp.where(i == n, jnp.int32(v), r)
    return r


def _late(h, i):
    return jnp.where((h == GROUP - 1) & (i == CHIPS - 2), GROUP, h)


def _kernel(x_hbm, gain_hbm, rot_hbm, off_hbm, wq, wk, wv, wo, y_hbm, xs, gain_ref, rot_ref, off_ref, a, cos_s, sin_s, wt, wos, kv_out, kv, q_out, qs, o_out, os, part, tops, yacc, y_part,
            x_sem, y_sem, table_sem, own_sem, ownq_sem, w_sem, wo_sem, kv_ss, kv_rs, rl_ss, q_ss, q_rs, o_ss, o_rs):
    me = lax.axis_index("sp")
    chip, core = me // 2, me % 2
    sibling = 2 * chip + 1 - core

    def other(mask):
        return jnp.bitwise_xor(chip, mask)

    def remote(src, dst, ss, rs, dev):
        return pltpu.make_async_remote_copy(src_ref=src, dst_ref=dst, send_sem=ss, recv_sem=rs, device_id={"sp": dev}, device_id_type=pl.DeviceIdType.MESH)

    def received(dst, sem):
        remote(dst, dst, sem, sem, sibling).wait_recv()

    def sent(src, sem):
        remote(src, src, sem, sem, sibling).wait_send()

    def x_copy(i):
        rows = pl.ds(i * (ROWS // X_PARTS), ROWS // X_PARTS)
        return pltpu.make_async_copy(x_hbm.at[rows], xs.at[rows], x_sem.at[i])

    gain_copy, rot_copy, off_copy = (pltpu.make_async_copy(src, dst, table_sem.at[n]) for n, (src, dst) in enumerate(
        ((gain_hbm, gain_ref), (rot_hbm, rot_ref), (off_hbm, off_ref))))
    gain_copy.start()
    for i in range(X_PARTS):
        x_copy(i).start()
    rot_copy.start()
    off_copy.start()

    def halves(slot, w0, at0, w1, at1):
        at0, at1 = pl.multiple_of(at0 * HEAD, HEAD), pl.multiple_of(at1 * HEAD, HEAD)
        return [pltpu.make_async_copy(w0.at[:, pl.ds(at0, HEAD)], wt.at[slot, :, pl.ds(0, HEAD)], w_sem.at[slot, 0]),
                pltpu.make_async_copy(w1.at[:, pl.ds(at1, HEAD)], wt.at[slot, :, pl.ds(HEAD, HEAD)], w_sem.at[slot, 1])]

    def kv_tile(slot, i):
        d = other(_pick(i, OUT))
        return halves(slot, wk, d, wv, d)

    def q_tile(slot, h, pair):
        d0, d1 = other(_pick(2 * pair, OUT)), other(_pick(2 * pair + 1, OUT))
        return halves(slot, wq, GROUP * d0 + h, wq, GROUP * d1 + h)

    def begin(copies):
        for c in copies:
            c.start()

    def start_tile(t):
        slot, first = t % SLOTS, t < 3 * CHIPS // 2

        @pl.when(first & (t % 3 < 2))
        def _():
            begin(kv_tile(slot, 2 * (t // 3) + t % 3))

        @pl.when(first & (t % 3 == 2))
        def _():
            begin(q_tile(slot, 0, t // 3))

        @pl.when((t >= 3 * CHIPS // 2) & (t < TILES))
        def _():
            j = t - 3 * CHIPS // 2
            begin(q_tile(slot, 1 + j // 4, j % 4))

    def wait_tile(t):
        for c in kv_tile(t % SLOTS, 0):
            c.wait()

    barrier = pltpu.get_barrier_semaphore()
    for m in range(1, CHIPS):
        pl.semaphore_signal(barrier, inc=1, device_id={"sp": 2 * other(m) + core}, device_id_type=pl.DeviceIdType.MESH)
    pl.semaphore_signal(barrier, inc=1, device_id={"sp": sibling}, device_id_type=pl.DeviceIdType.MESH)

    begin(kv_tile(0, 0))
    with jax.named_scope("norm"):
        gain_copy.wait()
        gain = gain_ref[...].reshape(1, D).astype(F32)
        for i in range(X_PARTS):
            x_copy(i).wait()
            if i == 0:
                begin(kv_tile(1, 1))
                begin(q_tile(2, 0, 0))
            rows = pl.ds(i * (ROWS // X_PARTS), ROWS // X_PARTS)
            wide = xs[rows, :].astype(F32)
            scale = lax.rsqrt(jnp.mean(wide * wide, -1, keepdims=True) + 1e-6)
            a[rows, :] = (wide * scale * gain).astype(BF16)
        begin(kv_tile(3, 2))
        begin(kv_tile(4, 3))
        begin(q_tile(5, 0, 1))

    with jax.named_scope("tables"):
        rot_copy.wait()
        off_copy.wait()
        c0, s0 = off_ref[0, pl.ds(me, 1), :], off_ref[1, pl.ds(me, 1), :]
        cos_s[...] = c0 * rot_ref[0] - s0 * rot_ref[1]
        sin = s0 * rot_ref[0] + c0 * rot_ref[1]
        sin_s[...] = jnp.where(lax.broadcasted_iota(jnp.int32, sin.shape, 1) < HALF, -sin, sin)
    def turned(t):
        t = t.astype(BF16).astype(F32)
        return (t * cos_s[...] + pltpu.roll(t, HALF, 1) * sin_s[...]).astype(BF16)

    def project(t, count):
        for n in range(count):
            with jax.named_scope("w_wait"):
                wait_tile(t + n)
        return [_dot(a[...], wt[(t + n) % SLOTS], 1, 0) for n in range(count)]

    def refill(t, count):
        for n in range(count):
            start_tile(jnp.int32(t + n + SLOTS))

    def kv_copy(i):
        return remote(kv_out.at[i], kv.at[me], kv_ss.at[0], kv_rs.at[me], 2 * other(_pick(i, OUT)) + core)

    def q_copy(h, i):
        return remote(q_out.at[h, i], qs.at[h, chip], q_ss.at[h], q_rs.at[chip if isinstance(h, int) and h == 0 else CHIPS + h], 2 * other(_pick(i, OUT)) + core)

    def keep_kv(i, r):
        k, v = turned(r[:, :HEAD]), r[:, HEAD:].astype(BF16).T
        kv_out[i, :ROWS, :] = k
        kv_out[i, ROWS : ROWS + HEAD, :] = v[:, :HEAD]
        kv_out[i, ROWS + HEAD :, :] = v[:, HEAD:]

    def keep_q(h, i, r):
        q_out[h, i] = turned(r[:, :HEAD])
        q_out[h, i + 1] = turned(r[:, HEAD:])

    def project_first(n, _):
        *rs, r = project(3 * n, 3)
        for i, kv_r in zip((2 * n, 2 * n + 1), rs):
            keep_kv(i, kv_r)
        keep_q(0, 2 * n, r)
        refill(3 * n, 3)
        kv_copy(2 * n).start()

        @pl.when(n < CHIPS // 2 - 1)
        def _():
            kv_copy(2 * n + 1).start()

        q_copy(0, 2 * n).start()

        @pl.when(n < CHIPS // 2 - 1)
        def _():
            q_copy(0, 2 * n + 1).start()

        return _

    with jax.named_scope("project_0"):
        keep_kv(0, project(0, 1)[0])
        with jax.named_scope("barrier"):
            pl.semaphore_wait(barrier, CHIPS)
        kv_copy(0).start()
        keep_kv(1, project(1, 1)[0])
        kv_copy(1).start()
        keep_q(0, 0, project(2, 1)[0])
        for i in range(2):
            q_copy(0, i).start()
        refill(0, 3)
    with jax.named_scope("project_first"):
        lax.fori_loop(1, CHIPS // 2, project_first, None)
    own_kv = pltpu.make_async_copy(kv_out.at[CHIPS - 1], kv.at[me], own_sem)
    own_kv.start()

    def relay(s):
        b = 2 * s + core
        return remote(kv.at[b], kv.at[b], rl_ss.at[0], kv_rs.at[b], sibling)

    def pass_on(p):
        s = other(_pick(p, IN))
        b = 2 * s + core
        remote(kv_out.at[0], kv.at[b], kv_ss.at[0], kv_rs.at[b], sibling).wait_recv()
        relay(s).start()

    def project_q(n, _):
        t = 2 * n + 3 * CHIPS // 2
        rs = project(t, 2)
        h, i0 = 1 + n // 2, 4 * (n % 2)
        for m, r in enumerate(rs):
            q_out[h, i0 + 2 * m] = turned(r[:, :HEAD])
            q_out[h, i0 + 2 * m + 1] = turned(r[:, HEAD:])
        refill(t, 2)
        for m in range(3):
            q_copy(h, i0 + m).start()

        @pl.when(n % 2 == 0)
        def _():
            q_copy(h, i0 + 3).start()

        return _

    with jax.named_scope("project_q"):
        own_kv.wait()
        relay(chip).start()
        lax.fori_loop(0, CHIPS // 2, project_q, None)
        own_q = [pltpu.make_async_copy(q_out.at[h, CHIPS - 1], qs.at[h, chip], ownq_sem.at[h]) for h in range(GROUP)]
        begin(own_q)
    with jax.named_scope("pass_on"):
        for p in (1, 2, 3):
            pass_on(p)

    def wo_copy(h, g):
        return pltpu.make_async_copy(wo.at[pl.ds((GROUP * g + h) * HEAD, HEAD), :], wos.at[h, pl.ds(g * HEAD, HEAD), :], wo_sem.at[h])

    for h in range(GROUP):
        for g in range(CHIPS):
            wo_copy(h, g).start()
    for c in own_q:
        c.wait()

    def arrive(p):
        s = other(_pick(p, IN))
        b = 2 * s + 1 - core
        remote(kv_out.at[0], kv.at[b], kv_ss.at[0], kv_rs.at[b], sibling).wait_recv()

        @pl.when(p > 0)
        def _():
            remote(q_out.at[0, 0], qs.at[0, s], q_ss.at[0], q_rs.at[s], sibling).wait_recv()

    def at(sq, sk):
        return sq * (sq + 1) // 2 + sk

    ones = jnp.ones((8, 2 * ROWS), BF16)

    def attend(h, items):
        scores = []
        for sq, sk, masked, _ in items:
            k = jnp.concatenate([kv[2 * sk, :ROWS, :], kv[2 * sk + 1, :ROWS, :]], axis=0)
            s = _dot(k, qs[h, sq], 1, 1)
            if masked:
                gap = lax.broadcasted_iota(jnp.int32, s.shape, 1) - lax.broadcasted_iota(jnp.int32, s.shape, 0)
                s = jnp.where(gap >= -ROWS * core, s, HIDDEN)
            scores.append(s)
        weights = []
        for (*_, to), s in zip(items, scores):
            top = s.max(axis=0, keepdims=True)
            tops[to] = jnp.broadcast_to(top, (8, ROWS))
            weights.append(jnp.exp2((s - top) * E).astype(BF16))
        for (_, sk, _, to), p in zip(items, weights):
            v = jnp.concatenate([kv[2 * sk + c, ROWS + n * HEAD : ROWS + (n + 1) * HEAD, :] for c in range(2) for n in range(2)], axis=1)
            part[to] = _dot(jnp.concatenate([v, ones], axis=0), p, 1, 0)

    def o_copy(h, i):
        sq = other(_pick(i, OUT))
        return remote(o_out.at[h, sq], os.at[h, chip], o_ss.at[h], o_rs.at[_late(h, i)], 2 * sq + core)

    def pair(s0, s1):
        sq, sk = jnp.maximum(s0, s1), jnp.minimum(s0, s1)
        return sq, sk, False, at(sq, sk)

    def first_head(n, _):
        with jax.named_scope("arrive"):
            arrive(2 * n)
            arrive(2 * n + 1)
        s0, s1 = other(_pick(2 * n, IN)), other(_pick(2 * n + 1, IN))
        attend(0, [(s0, s0, True, at(s0, s0)), (s1, s1, True, at(s1, s1)), pair(s0, s1)])

        def earlier(m, _):
            s2, s3 = other(_pick(2 * m, IN)), other(_pick(2 * m + 1, IN))
            attend(0, [pair(s, t) for t in (s2, s3) for s in (s0, s1)])
            return _

        with jax.named_scope("earlier"):
            lax.fori_loop(0, n, earlier, None)

        @pl.when((n == 0) | (n == 2))
        def _():
            with jax.named_scope("pass_on"):
                pass_on(n + 4)
                pass_on(n + 5)

        return _

    def finish(h, sq, slots, shown=None):
        t = [tops[n] for n in slots]
        if shown is not None:
            t = [jnp.where(show, x, HIDDEN) for show, x in zip(shown, t)]
        top = functools.reduce(jnp.maximum, t)
        acc = sum(part[n] * jnp.exp2((x - top) * E)[:1] for n, x in zip(slots, t))
        o_out[h, sq] = (acc[:HEAD] * (1 / acc[HEAD : HEAD + 1])).T.astype(BF16)

    with jax.named_scope("head_0"):
        lax.fori_loop(0, CHIPS // 2, first_head, None)
    with jax.named_scope("finish"):
        for sq in range(CHIPS):
            finish(0, sq, [at(sq, n) for n in range(sq + 1)])
        for i in range(CHIPS - 1):
            o_copy(0, i).start()

    def later_head(h, _):
        with jax.named_scope("q_wait"):
            received(qs.at[h, pl.ds(0, CHIPS - 1)], q_rs.at[CHIPS + h])

        def two(r, _):
            s0 = other(_pick(2 * r, OUT))
            big, small = jnp.maximum(s0, CHIPS - 1 - s0), jnp.minimum(s0, CHIPS - 1 - s0)
            items = [(big, big, True, 0), (small, small, True, 1)]
            for j in range(CHIPS - 1):
                items.append((jnp.where(j < big, big, small), jnp.where(j < big, j, j - big), False, j + 2))
            for n in range(0, len(items), STEP):
                attend(h, items[n : n + STEP])
            finish(h, big, (0, *range(2, 9)), [True, *(j < big for j in range(CHIPS - 1))])
            finish(h, small, (1, *range(2, 9)), [True, *(j >= big for j in range(CHIPS - 1))])
            o_copy(h, 2 * r).start()

            @pl.when(r < CHIPS // 2 - 1)
            def _():
                o_copy(h, 2 * r + 1).start()

            return _

        with jax.named_scope("rounds"):
            lax.fori_loop(0, CHIPS // 2, two, None)
        return _

    lax.fori_loop(1, GROUP, later_head, None)

    def y_copy(n):
        return pltpu.make_async_copy(y_part.at[n], y_hbm.at[:, pl.ds(pl.multiple_of(n * COLS, COLS), COLS)], y_sem.at[0])

    def columns(parts, first, last):
        def body(n, _):
            cols = pl.ds(pl.multiple_of(n * COLS, COLS), COLS)
            seen = jnp.concatenate([os[h, g] for h, g in parts], axis=1)
            w = jnp.concatenate([wos[h, pl.ds(pl.multiple_of(g * HEAD, HEAD), HEAD), cols] for h, g in parts], axis=0)
            r = _dot(seen, w, 1, 0)
            if not first:
                r += yacc[:, cols]
            if last:
                y_part[n] = (xs[:, cols].astype(F32) + r).astype(BF16)
                y_copy(n).start()
            else:
                yacc[:, cols] = r
            return _

        with jax.named_scope("columns"):
            lax.fori_loop(0, D // COLS, body, None)

    own_o = [pltpu.make_async_copy(o_out.at[h, chip], os.at[h, chip], ownq_sem.at[h]) for h in range(GROUP)]
    begin(own_o)
    for c in own_o:
        c.wait()
    with jax.named_scope("wo_wait"):
        for h in range(GROUP):
            pltpu.make_async_copy(wo.at[pl.ds(0, CHIPS * HEAD), :], wos.at[h], wo_sem.at[h]).wait()
    with jax.named_scope("o_wait"):
        received(os.at[0, pl.ds(0, CHIPS - 1)], o_rs.at[0])
        received(os.at[1, pl.ds(0, CHIPS - 1)], o_rs.at[1])
    columns([(h, g) for h in range(2) for g in range(CHIPS)], True, False)
    with jax.named_scope("o_wait"):
        received(os.at[2, pl.ds(0, CHIPS - 2)], o_rs.at[2])
    columns([(2, other(m)) for m in OUT[:-2]], False, False)
    with jax.named_scope("o_wait"):
        received(os.at[2, pl.ds(0, 1)], o_rs.at[GROUP])
    columns([(2, other(m)) for m in OUT[-2:]], False, True)
    pltpu.make_async_copy(y_part, y_part, y_sem.at[0]).wait()

    with jax.named_scope("sent"):
        sent(kv.at[pl.ds(0, CHIPS)], rl_ss.at[0])
        sent(kv_out.at[pl.ds(0, CHIPS - 1)], kv_ss.at[0])
        for h in range(GROUP):
            sent(q_out.at[h, pl.ds(0, CHIPS - 1)], q_ss.at[h])
            sent(o_out.at[h, pl.ds(0, CHIPS - 1)], o_ss.at[h])


def _tables():
    rate = float(THETA) ** (-np.arange(HALF) / HALF)
    def both(place):
        angle = np.tile(place[:, None] * rate, 2)
        return np.stack([np.cos(angle), np.sin(angle)]).astype(np.float32)
    return both(np.arange(ROWS, dtype=np.float64)), both(ROWS * np.arange(2 * CHIPS, dtype=np.float64))


def solution(mesh):
    rot, off = _tables()
    dma = pltpu.SemaphoreType.DMA
    anywhere, vmem = pl.BlockSpec(memory_space=pl.ANY), pl.BlockSpec(memory_space=pltpu.VMEM)

    def step(x, gain, wq, wk, wv, wo):
        block = (ROWS, HEAD)
        return pl.pallas_call(
            _kernel,
            out_shape=pltpu.VMEM((ROWS, D), BF16),
            in_specs=[anywhere] * 8,
            out_specs=anywhere,
            scratch_shapes=[
                pltpu.VMEM((ROWS, D), BF16),
                pltpu.VMEM((D,), BF16),
                pltpu.VMEM((2, *block), F32),
                pltpu.VMEM((2, 2 * CHIPS, HEAD), F32),
                pltpu.VMEM((ROWS, D), BF16),
                pltpu.VMEM(block, F32),
                pltpu.VMEM(block, F32),
                pltpu.VMEM((SLOTS, D, 2 * HEAD), BF16),
                pltpu.VMEM((GROUP, CHIPS * HEAD, D), BF16),
                pltpu.VMEM((CHIPS, 2 * ROWS, HEAD), BF16),
                pltpu.VMEM((2 * CHIPS, 2 * ROWS, HEAD), BF16),
                pltpu.VMEM((GROUP, CHIPS, *block), BF16),
                pltpu.VMEM((GROUP, CHIPS, *block), BF16),
                pltpu.VMEM((GROUP, CHIPS, *block), BF16),
                pltpu.VMEM((GROUP, CHIPS, *block), BF16),
                pltpu.VMEM((CHIPS * (CHIPS + 1) // 2, HEAD + 8, ROWS), F32),
                pltpu.VMEM((CHIPS * (CHIPS + 1) // 2, 8, ROWS), F32),
                pltpu.VMEM((ROWS, D), F32),
                pltpu.VMEM((D // COLS, ROWS, COLS), BF16),
                dma((X_PARTS,)),
                dma((1,)),
                dma((3,)),
                dma,
                dma((GROUP,)),
                dma((SLOTS, 2)),
                dma((GROUP,)),
                dma((1,)),
                dma((2 * CHIPS,)),
                dma((1,)),
                dma((GROUP,)),
                dma((CHIPS + GROUP,)),
                dma((GROUP,)),
                dma((GROUP + 1,)),
            ],
            compiler_params=pltpu.CompilerParams(collective_id=0, has_side_effects=True, vmem_limit_bytes=62 * 2**20),
        )(x, gain, jnp.asarray(rot), jnp.asarray(off), wq, wk, wv, wo)

    tokens, whole = P(("dp", "sp"), None), P(None, None)
    return jax.shard_map(
        step,
        mesh=mesh,
        in_specs=(tokens, P(None), whole, whole, whole, whole),
        out_specs=tokens,
        check_vma=False,
    )
```

```python
import functools

import jax
import jax.numpy as jnp
import numpy as np
from jax import lax
from jax.experimental import pallas as pl
from jax.experimental.pallas import tpu as pltpu
from jax.sharding import PartitionSpec as P

HEAD = 128
HALF = HEAD // 2
THETA = 10000
CHIPS = 8
GROUP = 3
ROWS = 256
D = 3072
HIDDEN = -2e30
E = HEAD**-0.5 * 1.4426950408889634
OUT = (6, 1, 5, 2, 3, 4, 7, 0)
IN = (0, 6, 1, 5, 2, 3, 4, 7)
SLOTS = 6
KV_TILES, Q_TILES = CHIPS, CHIPS * GROUP // 2
TILES = KV_TILES + Q_TILES
COLS = 1536
X_PARTS = 4
STEP = 9
LAG_W, LAG_P = 3, 5
F32, BF16 = jnp.float32, jnp.bfloat16


def _dot(a, b, ca, cb):
    return lax.dot_general(a, b, (((ca,), (cb,)), ((), ())), preferred_element_type=F32)


def _pick(i, table):
    r = jnp.int32(table[0])
    for n, v in enumerate(table[1:], 1):
        r = jnp.where(i == n, jnp.int32(v), r)
    return r


def _late(h, i):
    return jnp.where((h == GROUP - 1) & (i == CHIPS - 2), GROUP, h)


def _kernel(x_hbm, gain_hbm, rot_hbm, off_hbm, wq, wk, wv, wo, y_ref, xs, gain_ref, rot_ref, off_ref, a, cos_s, sin_s, wt, wos, kv_out, kv, q_out, qs, o_out, os, part, tops, yacc,
            x_sem, table_sem, own_sem, ownq_sem, w_sem, wo_sem, kv_ss, kv_rs, rl_ss, q_ss, q_rs, o_ss, o_rs):
    me = lax.axis_index("sp")
    chip, core = me // 2, me % 2
    sibling = 2 * chip + 1 - core

    def other(mask):
        return jnp.bitwise_xor(chip, mask)

    def remote(src, dst, ss, rs, dev):
        return pltpu.make_async_remote_copy(src_ref=src, dst_ref=dst, send_sem=ss, recv_sem=rs, device_id={"sp": dev}, device_id_type=pl.DeviceIdType.MESH)

    def received(dst, sem):
        remote(dst, dst, sem, sem, sibling).wait_recv()

    def sent(src, sem):
        remote(src, src, sem, sem, sibling).wait_send()

    def x_copy(i):
        rows = pl.ds(i * (ROWS // X_PARTS), ROWS // X_PARTS)
        return pltpu.make_async_copy(x_hbm.at[rows], xs.at[rows], x_sem.at[i])

    gain_copy, rot_copy, off_copy = (pltpu.make_async_copy(src, dst, table_sem.at[n]) for n, (src, dst) in enumerate(
        ((gain_hbm, gain_ref), (rot_hbm, rot_ref), (off_hbm, off_ref))))
    gain_copy.start()
    for i in range(X_PARTS):
        x_copy(i).start()
    rot_copy.start()
    off_copy.start()

    def halves(slot, w0, at0, w1, at1):
        at0, at1 = pl.multiple_of(at0 * HEAD, HEAD), pl.multiple_of(at1 * HEAD, HEAD)
        return [pltpu.make_async_copy(w0.at[:, pl.ds(at0, HEAD)], wt.at[slot, :, pl.ds(0, HEAD)], w_sem.at[slot, 0]),
                pltpu.make_async_copy(w1.at[:, pl.ds(at1, HEAD)], wt.at[slot, :, pl.ds(HEAD, HEAD)], w_sem.at[slot, 1])]

    def kv_tile(slot, i):
        d = other(_pick(i, OUT))
        return halves(slot, wk, d, wv, d)

    def q_tile(slot, h, pair):
        d0, d1 = other(_pick(2 * pair, OUT)), other(_pick(2 * pair + 1, OUT))
        return halves(slot, wq, GROUP * d0 + h, wq, GROUP * d1 + h)

    def begin(copies):
        for c in copies:
            c.start()

    def start_tile(t):
        slot, first = t % SLOTS, t < 3 * CHIPS // 2

        @pl.when(first & (t % 3 < 2))
        def _():
            begin(kv_tile(slot, 2 * (t // 3) + t % 3))

        @pl.when(first & (t % 3 == 2))
        def _():
            begin(q_tile(slot, 0, t // 3))

        @pl.when((t >= 3 * CHIPS // 2) & (t < TILES))
        def _():
            j = t - 3 * CHIPS // 2
            begin(q_tile(slot, 1 + j // 4, j % 4))

    def wait_tile(t):
        for c in kv_tile(t % SLOTS, 0):
            c.wait()

    barrier = pltpu.get_barrier_semaphore()
    for m in range(1, CHIPS):
        pl.semaphore_signal(barrier, inc=1, device_id={"sp": 2 * other(m) + core}, device_id_type=pl.DeviceIdType.MESH)
    pl.semaphore_signal(barrier, inc=1, device_id={"sp": sibling}, device_id_type=pl.DeviceIdType.MESH)

    begin(kv_tile(0, 0))
    with jax.named_scope("norm"):
        gain_copy.wait()
        gain = gain_ref[...].reshape(1, D).astype(F32)
        for i in range(X_PARTS):
            x_copy(i).wait()
            if i == 0:
                begin(kv_tile(1, 1))
                begin(q_tile(2, 0, 0))
            rows = pl.ds(i * (ROWS // X_PARTS), ROWS // X_PARTS)
            wide = xs[rows, :].astype(F32)
            scale = lax.rsqrt(jnp.mean(wide * wide, -1, keepdims=True) + 1e-6)
            a[rows, :] = (wide * scale * gain).astype(BF16)
        begin(kv_tile(3, 2))
        begin(kv_tile(4, 3))
        begin(q_tile(5, 0, 1))

    with jax.named_scope("tables"):
        rot_copy.wait()
        off_copy.wait()
        c0, s0 = off_ref[0, pl.ds(me, 1), :], off_ref[1, pl.ds(me, 1), :]
        cos_s[...] = c0 * rot_ref[0] - s0 * rot_ref[1]
        sin = s0 * rot_ref[0] + c0 * rot_ref[1]
        sin_s[...] = jnp.where(lax.broadcasted_iota(jnp.int32, sin.shape, 1) < HALF, -sin, sin)
    def turned(t):
        t = t.astype(BF16).astype(F32)
        return (t * cos_s[...] + pltpu.roll(t, HALF, 1) * sin_s[...]).astype(BF16)

    def project(t, count):
        for n in range(count):
            with jax.named_scope("w_wait"):
                wait_tile(t + n)
        return [_dot(a[...], wt[(t + n) % SLOTS], 1, 0) for n in range(count)]

    def refill(t, count):
        for n in range(count):
            start_tile(jnp.int32(t + n + SLOTS))

    def kv_copy(i):
        return remote(kv_out.at[i], kv.at[me], kv_ss.at[0], kv_rs.at[me], 2 * other(_pick(i, OUT)) + core)

    def q_copy(h, i):
        return remote(q_out.at[h, i], qs.at[h, chip], q_ss.at[h], q_rs.at[chip if isinstance(h, int) and h == 0 else CHIPS + h], 2 * other(_pick(i, OUT)) + core)

    def keep_kv(i, r):
        k, v = turned(r[:, :HEAD]), r[:, HEAD:].astype(BF16).T
        kv_out[i, :ROWS, :] = k
        kv_out[i, ROWS : ROWS + HEAD, :] = v[:, :HEAD]
        kv_out[i, ROWS + HEAD :, :] = v[:, HEAD:]

    def keep_q(h, i, r):
        q_out[h, i] = turned(r[:, :HEAD])
        q_out[h, i + 1] = turned(r[:, HEAD:])

    def project_first(n, _):
        *rs, r = project(3 * n, 3)
        for i, kv_r in zip((2 * n, 2 * n + 1), rs):
            keep_kv(i, kv_r)
        keep_q(0, 2 * n, r)
        refill(3 * n, 3)
        kv_copy(2 * n).start()

        @pl.when(n < CHIPS // 2 - 1)
        def _():
            kv_copy(2 * n + 1).start()

        q_copy(0, 2 * n).start()

        @pl.when(n < CHIPS // 2 - 1)
        def _():
            q_copy(0, 2 * n + 1).start()

        return _

    with jax.named_scope("project_0"):
        keep_kv(0, project(0, 1)[0])
        with jax.named_scope("barrier"):
            pl.semaphore_wait(barrier, CHIPS)
        kv_copy(0).start()
        keep_kv(1, project(1, 1)[0])
        kv_copy(1).start()
        keep_q(0, 0, project(2, 1)[0])
        for i in range(2):
            q_copy(0, i).start()
        refill(0, 3)
    with jax.named_scope("project_first"):
        lax.fori_loop(1, CHIPS // 2, project_first, None)
    own_kv = pltpu.make_async_copy(kv_out.at[CHIPS - 1], kv.at[me], own_sem)
    own_kv.start()

    def relay(s):
        b = 2 * s + core
        return remote(kv.at[b], kv.at[b], rl_ss.at[0], kv_rs.at[b], sibling)

    def pass_on(p):
        s = other(_pick(p, IN))
        b = 2 * s + core
        remote(kv_out.at[0], kv.at[b], kv_ss.at[0], kv_rs.at[b], sibling).wait_recv()
        relay(s).start()

    def project_q(n, _):
        t = 2 * n + 3 * CHIPS // 2
        rs = project(t, 2)
        h, i0 = 1 + n // 2, 4 * (n % 2)
        for m, r in enumerate(rs):
            q_out[h, i0 + 2 * m] = turned(r[:, :HEAD])
            q_out[h, i0 + 2 * m + 1] = turned(r[:, HEAD:])
        refill(t, 2)
        for m in range(3):
            q_copy(h, i0 + m).start()

        @pl.when(n % 2 == 0)
        def _():
            q_copy(h, i0 + 3).start()

        return _

    with jax.named_scope("project_q"):
        own_kv.wait()
        relay(chip).start()
        lax.fori_loop(0, CHIPS // 2, project_q, None)
        own_q = [pltpu.make_async_copy(q_out.at[h, CHIPS - 1], qs.at[h, chip], ownq_sem.at[h]) for h in range(GROUP)]
        begin(own_q)
    with jax.named_scope("pass_on"):
        for p in range(1, 6):
            pass_on(p)

    def wo_copy(h, g):
        return pltpu.make_async_copy(wo.at[pl.ds((GROUP * g + h) * HEAD, HEAD), :], wos.at[h, pl.ds(g * HEAD, HEAD), :], wo_sem.at[h])

    for h in range(GROUP):
        for g in range(CHIPS):
            wo_copy(h, g).start()
    for c in own_q:
        c.wait()

    def arrive(p):
        s = other(_pick(p, IN))
        b = 2 * s + 1 - core
        remote(kv_out.at[0], kv.at[b], kv_ss.at[0], kv_rs.at[b], sibling).wait_recv()

        @pl.when(p > 0)
        def _():
            remote(q_out.at[0, 0], qs.at[0, s], q_ss.at[0], q_rs.at[s], sibling).wait_recv()

    def at(sq, sk):
        return sq * (sq + 1) // 2 + sk

    ones = jnp.ones((8, 2 * ROWS), BF16)

    def attend(h, items):
        def score(sq, sk, masked, _):
            k = jnp.concatenate([kv[2 * sk, :ROWS, :], kv[2 * sk + 1, :ROWS, :]], axis=0)
            s = _dot(k, qs[h, sq], 1, 1)
            if masked:
                gap = lax.broadcasted_iota(jnp.int32, s.shape, 1) - lax.broadcasted_iota(jnp.int32, s.shape, 0)
                s = jnp.where(gap >= -ROWS * core, s, HIDDEN)
            return s

        def weigh(s, to):
            top = s.max(axis=0, keepdims=True)
            tops[to] = jnp.broadcast_to(top, (8, ROWS))
            return jnp.exp2((s - top) * E).astype(BF16)

        def add_up(p, sk, to):
            v = jnp.concatenate([kv[2 * sk + c, ROWS + n * HEAD : ROWS + (n + 1) * HEAD, :] for c in range(2) for n in range(2)], axis=1)
            part[to] = _dot(jnp.concatenate([v, ones], axis=0), p, 1, 0)

        s, p = {}, {}
        for n in range(len(items) + LAG_P):
            if n < len(items):
                s[n] = score(*items[n])
            if 0 <= n - LAG_W < len(items):
                m = n - LAG_W
                p[m] = weigh(s.pop(m), items[m][3])
            if 0 <= n - LAG_P < len(items):
                m = n - LAG_P
                add_up(p.pop(m), items[m][1], items[m][3])

    def o_copy(h, i):
        sq = other(_pick(i, OUT))
        return remote(o_out.at[h, sq], os.at[h, chip], o_ss.at[h], o_rs.at[_late(h, i)], 2 * sq + core)

    def pair(s0, s1):
        sq, sk = jnp.maximum(s0, s1), jnp.minimum(s0, s1)
        return sq, sk, False, at(sq, sk)

    def first_head(n, _):
        with jax.named_scope("arrive"):
            arrive(2 * n)
            arrive(2 * n + 1)
        s0, s1 = other(_pick(2 * n, IN)), other(_pick(2 * n + 1, IN))
        attend(0, [(s0, s0, True, at(s0, s0)), (s1, s1, True, at(s1, s1)), pair(s0, s1)])

        def earlier(m, _):
            s2, s3 = other(_pick(2 * m, IN)), other(_pick(2 * m + 1, IN))
            attend(0, [pair(s, t) for t in (s2, s3) for s in (s0, s1)])
            return _

        with jax.named_scope("earlier"):
            lax.fori_loop(0, n, earlier, None)

        @pl.when(n == 1)
        def _():
            with jax.named_scope("pass_on"):
                pass_on(6)
                pass_on(7)

        return _

    def finish(h, sq, slots, shown=None):
        t = [tops[n] for n in slots]
        if shown is not None:
            t = [jnp.where(show, x, HIDDEN) for show, x in zip(shown, t)]
        top = functools.reduce(jnp.maximum, t)
        acc = sum(part[n] * jnp.exp2((x - top) * E)[:1] for n, x in zip(slots, t))
        o_out[h, sq] = (acc[:HEAD] * (1 / acc[HEAD : HEAD + 1])).T.astype(BF16)

    with jax.named_scope("head_0"):
        lax.fori_loop(0, CHIPS // 2, first_head, None)
    with jax.named_scope("finish"):
        for sq in range(CHIPS):
            finish(0, sq, [at(sq, n) for n in range(sq + 1)])
        for i in range(CHIPS - 1):
            o_copy(0, i).start()

    def later_head(h, _):
        with jax.named_scope("q_wait"):
            received(qs.at[h, pl.ds(0, CHIPS - 1)], q_rs.at[CHIPS + h])

        def two(r, _):
            s0 = other(_pick(2 * r, OUT))
            big, small = jnp.maximum(s0, CHIPS - 1 - s0), jnp.minimum(s0, CHIPS - 1 - s0)
            items = [(big, big, True, 0), (small, small, True, 1)]
            for j in range(CHIPS - 1):
                items.append((jnp.where(j < big, big, small), jnp.where(j < big, j, j - big), False, j + 2))
            for n in range(0, len(items), STEP):
                attend(h, items[n : n + STEP])
            finish(h, big, (0, *range(2, 9)), [True, *(j < big for j in range(CHIPS - 1))])
            finish(h, small, (1, *range(2, 9)), [True, *(j >= big for j in range(CHIPS - 1))])
            o_copy(h, 2 * r).start()

            @pl.when(r < CHIPS // 2 - 1)
            def _():
                o_copy(h, 2 * r + 1).start()

            return _

        with jax.named_scope("rounds"):
            lax.fori_loop(0, CHIPS // 2, two, None)
        return _

    lax.fori_loop(1, GROUP, later_head, None)

    def columns(parts, first, last):
        def body(n, _):
            cols = pl.ds(pl.multiple_of(n * COLS, COLS), COLS)
            seen = jnp.concatenate([os[h, g] for h, g in parts], axis=1)
            w = jnp.concatenate([wos[h, pl.ds(pl.multiple_of(g * HEAD, HEAD), HEAD), cols] for h, g in parts], axis=0)
            r = _dot(seen, w, 1, 0)
            if not first:
                r += yacc[:, cols]
            if last:
                y_ref[:, cols] = (xs[:, cols].astype(F32) + r).astype(BF16)
            else:
                yacc[:, cols] = r
            return _

        with jax.named_scope("columns"):
            lax.fori_loop(0, D // COLS, body, None)

    own_o = [pltpu.make_async_copy(o_out.at[h, chip], os.at[h, chip], ownq_sem.at[h]) for h in range(GROUP)]
    begin(own_o)
    for c in own_o:
        c.wait()
    with jax.named_scope("wo_wait"):
        for h in range(GROUP):
            pltpu.make_async_copy(wo.at[pl.ds(0, CHIPS * HEAD), :], wos.at[h], wo_sem.at[h]).wait()
    with jax.named_scope("o_wait"):
        received(os.at[0, pl.ds(0, CHIPS - 1)], o_rs.at[0])
    columns([(0, g) for g in range(CHIPS)], True, False)
    with jax.named_scope("o_wait"):
        received(os.at[1, pl.ds(0, CHIPS - 1)], o_rs.at[1])
    columns([(1, g) for g in range(CHIPS)], False, False)
    with jax.named_scope("o_wait"):
        received(os.at[2, pl.ds(0, CHIPS - 2)], o_rs.at[2])
    columns([(2, other(m)) for m in OUT[:-2]], False, False)
    with jax.named_scope("o_wait"):
        received(os.at[2, pl.ds(0, 1)], o_rs.at[GROUP])
    columns([(2, other(m)) for m in OUT[-2:]], False, True)

    with jax.named_scope("sent"):
        sent(kv.at[pl.ds(0, CHIPS)], rl_ss.at[0])
        sent(kv_out.at[pl.ds(0, CHIPS - 1)], kv_ss.at[0])
        for h in range(GROUP):
            sent(q_out.at[h, pl.ds(0, CHIPS - 1)], q_ss.at[h])
            sent(o_out.at[h, pl.ds(0, CHIPS - 1)], o_ss.at[h])


def _tables():
    rate = float(THETA) ** (-np.arange(HALF) / HALF)
    def both(place):
        angle = np.tile(place[:, None] * rate, 2)
        return np.stack([np.cos(angle), np.sin(angle)]).astype(np.float32)
    return both(np.arange(ROWS, dtype=np.float64)), both(ROWS * np.arange(2 * CHIPS, dtype=np.float64))


def solution(mesh):
    rot, off = _tables()
    dma = pltpu.SemaphoreType.DMA
    anywhere, vmem = pl.BlockSpec(memory_space=pl.ANY), pl.BlockSpec(memory_space=pltpu.VMEM)

    def step(x, gain, wq, wk, wv, wo):
        block = (ROWS, HEAD)
        return pl.pallas_call(
            _kernel,
            out_shape=pltpu.VMEM((ROWS, D), BF16),
            in_specs=[anywhere] * 8,
            out_specs=vmem,
            scratch_shapes=[
                pltpu.VMEM((ROWS, D), BF16),
                pltpu.VMEM((D,), BF16),
                pltpu.VMEM((2, *block), F32),
                pltpu.VMEM((2, 2 * CHIPS, HEAD), F32),
                pltpu.VMEM((ROWS, D), BF16),
                pltpu.VMEM(block, F32),
                pltpu.VMEM(block, F32),
                pltpu.VMEM((SLOTS, D, 2 * HEAD), BF16),
                pltpu.VMEM((GROUP, CHIPS * HEAD, D), BF16),
                pltpu.VMEM((CHIPS, 2 * ROWS, HEAD), BF16),
                pltpu.VMEM((2 * CHIPS, 2 * ROWS, HEAD), BF16),
                pltpu.VMEM((GROUP, CHIPS, *block), BF16),
                pltpu.VMEM((GROUP, CHIPS, *block), BF16),
                pltpu.VMEM((GROUP, CHIPS, *block), BF16),
                pltpu.VMEM((GROUP, CHIPS, *block), BF16),
                pltpu.VMEM((CHIPS * (CHIPS + 1) // 2, HEAD + 8, ROWS), F32),
                pltpu.VMEM((CHIPS * (CHIPS + 1) // 2, 8, ROWS), F32),
                pltpu.VMEM((ROWS, D), F32),
                dma((X_PARTS,)),
                dma((3,)),
                dma,
                dma((GROUP,)),
                dma((SLOTS, 2)),
                dma((GROUP,)),
                dma((1,)),
                dma((2 * CHIPS,)),
                dma((1,)),
                dma((GROUP,)),
                dma((CHIPS + GROUP,)),
                dma((GROUP,)),
                dma((GROUP + 1,)),
            ],
            compiler_params=pltpu.CompilerParams(collective_id=0, has_side_effects=True, vmem_limit_bytes=62 * 2**20),
        )(x, gain, jnp.asarray(rot), jnp.asarray(off), wq, wk, wv, wo)

    tokens, whole = P(("dp", "sp"), None), P(None, None)
    return jax.shard_map(
        step,
        mesh=mesh,
        in_specs=(tokens, P(None), whole, whole, whole, whole),
        out_specs=tokens,
        check_vma=False,
    )
```

```python
import functools

import jax
import jax.numpy as jnp
import numpy as np
from jax import lax
from jax.experimental import pallas as pl
from jax.experimental.pallas import tpu as pltpu
from jax.sharding import PartitionSpec as P

HEAD = 128
HALF = HEAD // 2
THETA = 10000
CHIPS = 8
GROUP = 3
ROWS = 256
D = 3072
HIDDEN = -2e30
E = HEAD**-0.5 * 1.4426950408889634
OUT = (6, 1, 5, 2, 3, 4, 7, 0)
IN = (0, 6, 1, 5, 2, 3, 4, 7)
LATE = ((1, 3, 4), (1, 3, 4))
SLOTS = 6
KV_TILES, Q_TILES = CHIPS, CHIPS * GROUP // 2
TILES = KV_TILES + Q_TILES
COLS = 1536
X_PARTS = 4
STEP = 9
LAG_W, LAG_P = 3, 5
F32, BF16 = jnp.float32, jnp.bfloat16


def _dot(a, b, ca, cb):
    return lax.dot_general(a, b, (((ca,), (cb,)), ((), ())), preferred_element_type=F32)


def _pick(i, table):
    r = jnp.int32(table[0])
    for n, v in enumerate(table[1:], 1):
        r = jnp.where(i == n, jnp.int32(v), r)
    return r


KV_BATCH = (0, 0, 0, 0, 0, 1, 1, 1)
Q_BATCH = (0, 1, 1, 2, 2, 3, 3, 0)


def _batch(i, table):
    return table[i] if isinstance(i, int) else _pick(i, table)


def _late(h, i):
    return jnp.where((h == GROUP - 1) & (i == CHIPS - 2), GROUP, h)


def _kernel(x_hbm, gain_hbm, rot_hbm, off_hbm, wq, wk, wv, wo, y_ref, xs, gain_ref, rot_ref, off_ref, a, cos_s, sin_s, wt, wos, kv_out, kv, q_out, qs, o_out, os, part, tops, yacc,
            x_sem, table_sem, own_sem, ownq_sem, w_sem, wo_sem, kv_ss, kv_rs, rl_ss, q_ss, q_rs, o_ss, o_rs):
    me = lax.axis_index("sp")
    chip, core = me // 2, me % 2
    sibling = 2 * chip + 1 - core

    def other(mask):
        return jnp.bitwise_xor(chip, mask)

    def remote(src, dst, ss, rs, dev):
        return pltpu.make_async_remote_copy(src_ref=src, dst_ref=dst, send_sem=ss, recv_sem=rs, device_id={"sp": dev}, device_id_type=pl.DeviceIdType.MESH)

    def received(dst, sem):
        remote(dst, dst, sem, sem, sibling).wait_recv()

    def sent(src, sem):
        remote(src, src, sem, sem, sibling).wait_send()

    def done(ref, sem):
        pltpu.make_async_copy(ref, ref, sem).wait()

    def x_copy(i):
        rows = pl.ds(i * (ROWS // X_PARTS), ROWS // X_PARTS)
        return pltpu.make_async_copy(x_hbm.at[rows], xs.at[rows], x_sem.at[i])

    gain_copy, rot_copy, off_copy = (pltpu.make_async_copy(src, dst, table_sem.at[n]) for n, (src, dst) in enumerate(
        ((gain_hbm, gain_ref), (rot_hbm, rot_ref), (off_hbm, off_ref))))
    gain_copy.start()
    for i in range(X_PARTS):
        x_copy(i).start()
    rot_copy.start()
    off_copy.start()

    def halves(slot, w0, at0, w1, at1):
        at0, at1 = pl.multiple_of(at0 * HEAD, HEAD), pl.multiple_of(at1 * HEAD, HEAD)
        return [pltpu.make_async_copy(w0.at[:, pl.ds(at0, HEAD)], wt.at[slot, :, pl.ds(0, HEAD)], w_sem.at[slot]),
                pltpu.make_async_copy(w1.at[:, pl.ds(at1, HEAD)], wt.at[slot, :, pl.ds(HEAD, HEAD)], w_sem.at[slot])]

    def kv_tile(slot, i):
        d = other(_pick(i, OUT))
        return halves(slot, wk, d, wv, d)

    def q_tile(slot, h, pair):
        d0, d1 = other(_pick(2 * pair, OUT)), other(_pick(2 * pair + 1, OUT))
        return halves(slot, wq, GROUP * d0 + h, wq, GROUP * d1 + h)

    def begin(copies):
        for c in copies:
            c.start()

    def start_tile(t):
        slot, first = t % SLOTS, t < 3 * CHIPS // 2

        @pl.when(first & (t % 3 < 2))
        def _():
            begin(kv_tile(slot, 2 * (t // 3) + t % 3))

        @pl.when(first & (t % 3 == 2))
        def _():
            begin(q_tile(slot, 0, t // 3))

        @pl.when((t >= 3 * CHIPS // 2) & (t < TILES))
        def _():
            j = t - 3 * CHIPS // 2
            begin(q_tile(slot, 1 + j // 4, j % 4))

    def wait_tile(t):
        done(wt.at[t % SLOTS], w_sem.at[t % SLOTS])

    barrier = pltpu.get_barrier_semaphore()
    for m in range(1, CHIPS):
        pl.semaphore_signal(barrier, inc=1, device_id={"sp": 2 * other(m) + core}, device_id_type=pl.DeviceIdType.MESH)
    pl.semaphore_signal(barrier, inc=1, device_id={"sp": sibling}, device_id_type=pl.DeviceIdType.MESH)

    d0, d1 = other(OUT[0]), other(OUT[1])
    begin(halves(0, wk, d0, wk, d1))
    with jax.named_scope("norm"):
        gain_copy.wait()
        gain = gain_ref[...].reshape(1, D).astype(F32)
        for i in range(X_PARTS):
            x_copy(i).wait()
            if i == 0:
                begin(halves(1, wv, d0, wv, d1))
                begin(q_tile(2, 0, 0))
            rows = pl.ds(i * (ROWS // X_PARTS), ROWS // X_PARTS)
            wide = xs[rows, :].astype(F32)
            scale = lax.rsqrt(jnp.mean(wide * wide, -1, keepdims=True) + 1e-6)
            a[rows, :] = (wide * scale * gain).astype(BF16)
        begin(kv_tile(3, 2))
        begin(kv_tile(4, 3))
        begin(q_tile(5, 0, 1))

    with jax.named_scope("tables"):
        rot_copy.wait()
        off_copy.wait()
        c0, s0 = off_ref[0, pl.ds(me, 1), :], off_ref[1, pl.ds(me, 1), :]
        cos_s[...] = c0 * rot_ref[0] - s0 * rot_ref[1]
        sin = s0 * rot_ref[0] + c0 * rot_ref[1]
        sin_s[...] = jnp.where(lax.broadcasted_iota(jnp.int32, sin.shape, 1) < HALF, -sin, sin)
    def turned(t):
        t = t.astype(BF16).astype(F32)
        return (t * cos_s[...] + pltpu.roll(t, HALF, 1) * sin_s[...]).astype(BF16)

    def project(t, count):
        for n in range(count):
            with jax.named_scope("w_wait"):
                wait_tile(t + n)
        return [_dot(a[...], wt[(t + n) % SLOTS], 1, 0) for n in range(count)]

    def refill(t, count):
        for n in range(count):
            start_tile(jnp.int32(t + n + SLOTS))

    def kv_copy(i, rows=pl.ds(0, 2 * ROWS)):
        return remote(kv_out.at[i, rows], kv.at[me, rows], kv_ss.at[0], kv_rs.at[_batch(i, KV_BATCH)], 2 * other(_pick(i, OUT)) + core)

    def q_copy(h, i):
        return remote(q_out.at[h, i], qs.at[h, chip], q_ss.at[0], q_rs.at[_batch(i, Q_BATCH) if isinstance(h, int) and h == 0 else 3 + h], 2 * other(_pick(i, OUT)) + core)

    def keep_k(i, r):
        kv_out[i, :ROWS, :] = turned(r)

    def keep_v(i, r):
        v = r.astype(BF16).T
        kv_out[i, ROWS : ROWS + HEAD, :] = v[:, :HEAD]
        kv_out[i, ROWS + HEAD :, :] = v[:, HEAD:]

    def keep_q(h, i, r):
        q_out[h, i] = turned(r[:, :HEAD])
        q_out[h, i + 1] = turned(r[:, HEAD:])

    def project_first(n, _):
        *rs, r = project(3 * n, 3)
        for i, kv_r in zip((2 * n, 2 * n + 1), rs):
            keep_k(i, kv_r[:, :HEAD])
            keep_v(i, kv_r[:, HEAD:])
        keep_q(0, 2 * n, r)
        refill(3 * n, 3)
        kv_copy(2 * n).start()

        @pl.when(n < CHIPS // 2 - 1)
        def _():
            kv_copy(2 * n + 1).start()

        q_copy(0, 2 * n).start()

        @pl.when(n < CHIPS // 2 - 1)
        def _():
            q_copy(0, 2 * n + 1).start()

        return _

    with jax.named_scope("project_0"):
        r = project(0, 1)[0]
        for i in range(2):
            keep_k(i, r[:, i * HEAD : (i + 1) * HEAD])
        with jax.named_scope("barrier"):
            pl.semaphore_wait(barrier, CHIPS)
        for i in range(2):
            kv_copy(i, pl.ds(0, ROWS)).start()
        r = project(1, 1)[0]
        for i in range(2):
            keep_v(i, r[:, i * HEAD : (i + 1) * HEAD])
            kv_copy(i, pl.ds(ROWS, ROWS)).start()
        keep_q(0, 0, project(2, 1)[0])
        for i in range(2):
            q_copy(0, i).start()
        refill(0, 3)
    with jax.named_scope("project_first"):
        lax.fori_loop(1, CHIPS // 2, project_first, None)
    own_kv = pltpu.make_async_copy(kv_out.at[CHIPS - 1], kv.at[me], own_sem)
    own_kv.start()

    def relay(p):
        b = 2 * other(IN[p]) + core
        return remote(kv.at[b], kv.at[b], rl_ss.at[0], kv_rs.at[2 + p // 2], sibling)

    def pass_on(batch):
        received(kv.at[pl.ds(0, KV_BATCH[:-1].count(batch))], kv_rs.at[batch])
        for p in ((1, 2, 3, 4, 5), (6, 7))[batch]:
            relay(p).start()

    def project_q(n, _):
        t = 2 * n + 3 * CHIPS // 2
        rs = project(t, 2)
        h, i0 = 1 + n // 2, 4 * (n % 2)
        for m, r in enumerate(rs):
            q_out[h, i0 + 2 * m] = turned(r[:, :HEAD])
            q_out[h, i0 + 2 * m + 1] = turned(r[:, HEAD:])
        refill(t, 2)
        for m in range(4):
            early = [[i for i in range(CHIPS - 1) if i not in late] for late in LATE]
            for first in (0, 4):
                hs = [h_ for h_ in (1, 2) if first + m in early[h_ - 1]]
                if hs:
                    @pl.when((i0 == first) & ((h == hs[0]) | (h == hs[-1])))
                    def _():
                        q_copy(h, first + m).start()

        return _

    with jax.named_scope("project_q"):
        own_kv.wait()
        relay(0).start()
        lax.fori_loop(0, CHIPS // 2, project_q, None)
        own_q = [pltpu.make_async_copy(q_out.at[h, CHIPS - 1], qs.at[h, chip], ownq_sem) for h in range(GROUP)]
        begin(own_q)
    with jax.named_scope("pass_on"):
        pass_on(0)

    def wo_copy(h, g):
        return pltpu.make_async_copy(wo.at[pl.ds((GROUP * g + h) * HEAD, HEAD), :], wos.at[h, pl.ds(g * HEAD, HEAD), :], wo_sem.at[h])

    for h in range(GROUP):
        for g in range(CHIPS):
            wo_copy(h, g).start()
    done(qs.at[pl.ds(0, GROUP), 0], ownq_sem)

    def arrive(n):
        received(kv.at[pl.ds(0, 2)], kv_rs.at[2 + n])

        @pl.when(n == 0)
        def _():
            received(qs.at[0, pl.ds(0, 1)], q_rs.at[0])

        @pl.when(n > 0)
        def _():
            received(qs.at[0, pl.ds(0, 2)], q_rs.at[n])

    def at(sq, sk):
        return sq * (sq + 1) // 2 + sk

    ones = jnp.ones((8, 2 * ROWS), BF16)

    def attend(h, items):
        def score(sq, sk, masked, _):
            k = jnp.concatenate([kv[2 * sk, :ROWS, :], kv[2 * sk + 1, :ROWS, :]], axis=0)
            s = _dot(k, qs[h, sq], 1, 1)
            if masked:
                gap = lax.broadcasted_iota(jnp.int32, s.shape, 1) - lax.broadcasted_iota(jnp.int32, s.shape, 0)
                s = jnp.where(gap >= -ROWS * core, s, HIDDEN)
            return s

        def weigh(s, to):
            top = s.max(axis=0, keepdims=True)
            tops[to] = jnp.broadcast_to(top, (8, ROWS))
            return jnp.exp2((s - top) * E).astype(BF16)

        def add_up(p, sk, to):
            v = jnp.concatenate([kv[2 * sk + c, ROWS + n * HEAD : ROWS + (n + 1) * HEAD, :] for c in range(2) for n in range(2)], axis=1)
            part[to] = _dot(jnp.concatenate([v, ones], axis=0), p, 1, 0)

        s, p = {}, {}
        for n in range(len(items) + LAG_P):
            if n < len(items):
                s[n] = score(*items[n])
            if 0 <= n - LAG_W < len(items):
                m = n - LAG_W
                p[m] = weigh(s.pop(m), items[m][3])
            if 0 <= n - LAG_P < len(items):
                m = n - LAG_P
                add_up(p.pop(m), items[m][1], items[m][3])

    def o_copy(h, i):
        sq = other(_pick(i, OUT))
        return remote(o_out.at[h, sq], os.at[h, chip], o_ss.at[0], o_rs.at[_late(h, i)], 2 * sq + core)

    def pair(s0, s1):
        sq, sk = jnp.maximum(s0, s1), jnp.minimum(s0, s1)
        return sq, sk, False, at(sq, sk)

    def first_head(n, _):
        with jax.named_scope("arrive"):
            arrive(n)
        s0, s1 = other(_pick(2 * n, IN)), other(_pick(2 * n + 1, IN))
        attend(0, [(s0, s0, True, at(s0, s0)), (s1, s1, True, at(s1, s1)), pair(s0, s1)])

        def earlier(m, _):
            s2, s3 = other(_pick(2 * m, IN)), other(_pick(2 * m + 1, IN))
            attend(0, [pair(s, t) for t in (s2, s3) for s in (s0, s1)])
            return _

        with jax.named_scope("earlier"):
            lax.fori_loop(0, n, earlier, None)

        @pl.when(n == 1)
        def _():
            with jax.named_scope("pass_on"):
                pass_on(1)

        @pl.when(n == 0)
        def _():
            for h, late in enumerate(LATE, 1):
                for i in late:
                    q_copy(h, i).start()

        return _

    def finish(h, sq, slots, shown=None):
        t = [tops[n] for n in slots]
        if shown is not None:
            t = [jnp.where(show, x, HIDDEN) for show, x in zip(shown, t)]
        top = functools.reduce(jnp.maximum, t)
        acc = sum(part[n] * jnp.exp2((x - top) * E)[:1] for n, x in zip(slots, t))
        o_out[h, sq] = (acc[:HEAD] * (1 / acc[HEAD : HEAD + 1])).T.astype(BF16)

    with jax.named_scope("head_0"):
        lax.fori_loop(0, CHIPS // 2, first_head, None)
    with jax.named_scope("finish"):
        for sq in range(CHIPS):
            finish(0, sq, [at(sq, n) for n in range(sq + 1)])
        for i in range(CHIPS - 1):
            o_copy(0, i).start()

    def later_head(h, _):
        with jax.named_scope("q_wait"):
            received(qs.at[h, pl.ds(0, CHIPS - 1)], q_rs.at[3 + h])

        def two(r, _):
            s0 = other(_pick(2 * r, OUT))
            big, small = jnp.maximum(s0, CHIPS - 1 - s0), jnp.minimum(s0, CHIPS - 1 - s0)
            items = [(big, big, True, 0), (small, small, True, 1)]
            for j in range(CHIPS - 1):
                items.append((jnp.where(j < big, big, small), jnp.where(j < big, j, j - big), False, j + 2))
            for n in range(0, len(items), STEP):
                attend(h, items[n : n + STEP])
            finish(h, big, (0, *range(2, 9)), [True, *(j < big for j in range(CHIPS - 1))])
            finish(h, small, (1, *range(2, 9)), [True, *(j >= big for j in range(CHIPS - 1))])
            o_copy(h, 2 * r).start()

            @pl.when(r < CHIPS // 2 - 1)
            def _():
                o_copy(h, 2 * r + 1).start()

            return _

        with jax.named_scope("rounds"):
            lax.fori_loop(0, CHIPS // 2, two, None)
        return _

    lax.fori_loop(1, GROUP, later_head, None)

    def columns(parts, first, last):
        def body(n, _):
            cols = pl.ds(pl.multiple_of(n * COLS, COLS), COLS)
            seen = jnp.concatenate([os[h, g] for h, g in parts], axis=1)
            w = jnp.concatenate([wos[h, pl.ds(pl.multiple_of(g * HEAD, HEAD), HEAD), cols] for h, g in parts], axis=0)
            r = _dot(seen, w, 1, 0)
            r += xs[:, cols].astype(F32) if first else yacc[:, cols]
            if last:
                y_ref[:, cols] = r.astype(BF16)
            else:
                yacc[:, cols] = r
            return _

        with jax.named_scope("columns"):
            lax.fori_loop(0, D // COLS, body, None)

    own_o = [pltpu.make_async_copy(o_out.at[h, chip], os.at[h, chip], ownq_sem) for h in range(GROUP)]
    begin(own_o)
    done(os.at[pl.ds(0, GROUP), 0], ownq_sem)
    with jax.named_scope("wo_wait"):
        for h in range(GROUP):
            pltpu.make_async_copy(wo.at[pl.ds(0, CHIPS * HEAD), :], wos.at[h], wo_sem.at[h]).wait()
    with jax.named_scope("o_wait"):
        received(os.at[0, pl.ds(0, CHIPS - 1)], o_rs.at[0])
    columns([(0, g) for g in range(CHIPS)], True, False)
    with jax.named_scope("o_wait"):
        received(os.at[1, pl.ds(0, CHIPS - 1)], o_rs.at[1])
    columns([(1, g) for g in range(CHIPS)], False, False)
    with jax.named_scope("o_wait"):
        received(os.at[2, pl.ds(0, CHIPS - 2)], o_rs.at[2])
    columns([(2, other(m)) for m in OUT[:-2]], False, False)
    with jax.named_scope("o_wait"):
        received(os.at[2, pl.ds(0, 1)], o_rs.at[GROUP])
    columns([(2, other(m)) for m in OUT[-2:]], False, True)

    with jax.named_scope("sent"):
        sent(kv.at[pl.ds(0, CHIPS)], rl_ss.at[0])
        sent(kv_out.at[pl.ds(0, CHIPS - 1)], kv_ss.at[0])
        sent(q_out.at[pl.ds(0, GROUP), pl.ds(0, CHIPS - 1)], q_ss.at[0])
        sent(o_out.at[pl.ds(0, GROUP), pl.ds(0, CHIPS - 1)], o_ss.at[0])


def _tables():
    rate = float(THETA) ** (-np.arange(HALF) / HALF)
    def both(place):
        angle = np.tile(place[:, None] * rate, 2)
        return np.stack([np.cos(angle), np.sin(angle)]).astype(np.float32)
    return both(np.arange(ROWS, dtype=np.float64)), both(ROWS * np.arange(2 * CHIPS, dtype=np.float64))


def solution(mesh):
    rot, off = _tables()
    dma = pltpu.SemaphoreType.DMA
    anywhere, vmem = pl.BlockSpec(memory_space=pl.ANY), pl.BlockSpec(memory_space=pltpu.VMEM)

    def step(x, gain, wq, wk, wv, wo):
        block = (ROWS, HEAD)
        return pl.pallas_call(
            _kernel,
            out_shape=pltpu.VMEM((ROWS, D), BF16),
            in_specs=[anywhere] * 8,
            out_specs=vmem,
            scratch_shapes=[
                pltpu.VMEM((ROWS, D), BF16),
                pltpu.VMEM((D,), BF16),
                pltpu.VMEM((2, *block), F32),
                pltpu.VMEM((2, 2 * CHIPS, HEAD), F32),
                pltpu.VMEM((ROWS, D), BF16),
                pltpu.VMEM(block, F32),
                pltpu.VMEM(block, F32),
                pltpu.VMEM((SLOTS, D, 2 * HEAD), BF16),
                pltpu.VMEM((GROUP, CHIPS * HEAD, D), BF16),
                pltpu.VMEM((CHIPS, 2 * ROWS, HEAD), BF16),
                pltpu.VMEM((2 * CHIPS, 2 * ROWS, HEAD), BF16),
                pltpu.VMEM((GROUP, CHIPS, *block), BF16),
                pltpu.VMEM((GROUP, CHIPS, *block), BF16),
                pltpu.VMEM((GROUP, CHIPS, *block), BF16),
                pltpu.VMEM((GROUP, CHIPS, *block), BF16),
                pltpu.VMEM((CHIPS * (CHIPS + 1) // 2, HEAD + 8, ROWS), F32),
                pltpu.VMEM((CHIPS * (CHIPS + 1) // 2, 8, ROWS), F32),
                pltpu.VMEM((ROWS, D), F32),
                dma((X_PARTS,)),
                dma((3,)),
                dma,
                dma,
                dma((SLOTS,)),
                dma((GROUP,)),
                dma((1,)),
                dma((2 + CHIPS // 2,)),
                dma((1,)),
                dma((1,)),
                dma((CHIPS // 2 + GROUP - 1,)),
                dma((1,)),
                dma((GROUP + 1,)),
            ],
            compiler_params=pltpu.CompilerParams(collective_id=0, has_side_effects=True, vmem_limit_bytes=62 * 2**20),
        )(x, gain, jnp.asarray(rot), jnp.asarray(off), wq, wk, wv, wo)

    tokens, whole = P(("dp", "sp"), None), P(None, None)
    return jax.shard_map(
        step,
        mesh=mesh,
        in_specs=(tokens, P(None), whole, whole, whole, whole),
        out_specs=tokens,
        check_vma=False,
    )
```

```python
import functools

import jax
import jax.numpy as jnp
import numpy as np
from jax import lax
from jax.experimental import pallas as pl
from jax.experimental.pallas import tpu as pltpu
from jax.sharding import PartitionSpec as P

HEAD = 128
HALF = HEAD // 2
THETA = 10000
CHIPS = 8
GROUP = 3
ROWS = 256
D = 3072
HIDDEN = -3e38
E = HEAD**-0.5 * 1.4426950408889634
OUT = (6, 1, 5, 2, 3, 4, 7, 0)
IN = (0, 6, 1, 5, 2, 3, 4, 7)
LATE = ((1, 3, 4), (1, 3, 4))
PARTS = (0, 4, 6, 8)
SLOTS = 6
KV_TILES, Q_TILES = CHIPS, CHIPS * GROUP // 2
TILES = KV_TILES + Q_TILES
COLS = 1536
X_PARTS = 4
STEP = 9
LAG_W, LAG_P = 3, 5
F32, BF16 = jnp.float32, jnp.bfloat16


def _dot(a, b, ca, cb):
    return lax.dot_general(a, b, (((ca,), (cb,)), ((), ())), preferred_element_type=F32)


def _pick(i, table):
    r = jnp.int32(table[0])
    for n, v in enumerate(table[1:], 1):
        r = jnp.where(i == n, jnp.int32(v), r)
    return r


KV_BATCH = (0, 0, 0, 0, 0, 1, 1, 1)
Q_BATCH = (0, 1, 1, 2, 2, 3, 3, 0)


def _batch(i, table):
    return table[i] if isinstance(i, int) else _pick(i, table)


def _late(h, i):
    return jnp.where(h == GROUP - 1, h + sum(jnp.where(i >= p, 1, 0) for p in PARTS[1:-1]), h)


def _kernel(x_hbm, gain_hbm, rot_hbm, off_hbm, wq, wk, wv, wo, y_ref, xs, gain_ref, rot_ref, off_ref, a, cos_s, sin_s, wt, wos, kv_out, kv, q_out, qs, o_out, os, part, tops, yacc,
            x_sem, table_sem, own_sem, ownq_sem, w_sem, wo_sem, kv_ss, kv_rs, rl_ss, q_ss, q_rs, o_ss, o_rs):
    me = lax.axis_index("sp")
    chip, core = me // 2, me % 2
    sibling = 2 * chip + 1 - core

    def other(mask):
        return jnp.bitwise_xor(chip, mask)

    def remote(src, dst, ss, rs, dev):
        return pltpu.make_async_remote_copy(src_ref=src, dst_ref=dst, send_sem=ss, recv_sem=rs, device_id={"sp": dev}, device_id_type=pl.DeviceIdType.MESH)

    def received(dst, sem):
        remote(dst, dst, sem, sem, sibling).wait_recv()

    def sent(src, sem):
        remote(src, src, sem, sem, sibling).wait_send()

    def done(ref, sem):
        pltpu.make_async_copy(ref, ref, sem).wait()

    def x_copy(i):
        rows = pl.ds(i * (ROWS // X_PARTS), ROWS // X_PARTS)
        return pltpu.make_async_copy(x_hbm.at[rows], xs.at[rows], x_sem.at[i])

    gain_copy, rot_copy, off_copy = (pltpu.make_async_copy(src, dst, table_sem.at[n]) for n, (src, dst) in enumerate(
        ((gain_hbm, gain_ref), (rot_hbm, rot_ref), (off_hbm, off_ref))))
    gain_copy.start()
    for i in range(X_PARTS):
        x_copy(i).start()
    rot_copy.start()
    off_copy.start()

    def halves(slot, w0, at0, w1, at1):
        at0, at1 = pl.multiple_of(at0 * HEAD, HEAD), pl.multiple_of(at1 * HEAD, HEAD)
        return [pltpu.make_async_copy(w0.at[:, pl.ds(at0, HEAD)], wt.at[slot, :, pl.ds(0, HEAD)], w_sem.at[slot]),
                pltpu.make_async_copy(w1.at[:, pl.ds(at1, HEAD)], wt.at[slot, :, pl.ds(HEAD, HEAD)], w_sem.at[slot])]

    def kv_tile(slot, i):
        d = other(_pick(i, OUT))
        return halves(slot, wk, d, wv, d)

    def q_tile(slot, h, pair):
        d0, d1 = other(_pick(2 * pair, OUT)), other(_pick(2 * pair + 1, OUT))
        return halves(slot, wq, GROUP * d0 + h, wq, GROUP * d1 + h)

    def begin(copies):
        for c in copies:
            c.start()

    def start_tile(t):
        slot, first = t % SLOTS, t < 3 * CHIPS // 2

        @pl.when(first & (t % 3 < 2))
        def _():
            begin(kv_tile(slot, 2 * (t // 3) + t % 3))

        @pl.when(first & (t % 3 == 2))
        def _():
            begin(q_tile(slot, 0, t // 3))

        @pl.when((t >= 3 * CHIPS // 2) & (t < TILES))
        def _():
            j = t - 3 * CHIPS // 2
            begin(q_tile(slot, 1 + j // 4, j % 4))

    def wait_tile(t):
        done(wt.at[t % SLOTS], w_sem.at[t % SLOTS])

    barrier = pltpu.get_barrier_semaphore()
    for m in range(1, CHIPS):
        pl.semaphore_signal(barrier, inc=1, device_id={"sp": 2 * other(m) + core}, device_id_type=pl.DeviceIdType.MESH)
    pl.semaphore_signal(barrier, inc=1, device_id={"sp": sibling}, device_id_type=pl.DeviceIdType.MESH)

    d0, d1 = other(OUT[0]), other(OUT[1])
    begin(halves(0, wk, d0, wk, d1))
    with jax.named_scope("norm"):
        gain_copy.wait()
        gain = gain_ref[...].reshape(1, D).astype(F32)
        for i in range(X_PARTS):
            x_copy(i).wait()
            if i == 0:
                begin(halves(1, wv, d0, wv, d1))
                begin(q_tile(2, 0, 0))
            rows = pl.ds(i * (ROWS // X_PARTS), ROWS // X_PARTS)
            wide = xs[rows, :].astype(F32)
            scale = lax.rsqrt(jnp.mean(wide * wide, -1, keepdims=True) + 1e-6)
            a[rows, :] = (wide * scale * gain).astype(BF16)
        begin(kv_tile(3, 2))
        begin(kv_tile(4, 3))
        begin(q_tile(5, 0, 1))

    with jax.named_scope("tables"):
        rot_copy.wait()
        off_copy.wait()
        c0, s0 = off_ref[0, pl.ds(me, 1), :], off_ref[1, pl.ds(me, 1), :]
        cos_s[...] = c0 * rot_ref[0] - s0 * rot_ref[1]
        sin = s0 * rot_ref[0] + c0 * rot_ref[1]
        sin_s[...] = jnp.where(lax.broadcasted_iota(jnp.int32, sin.shape, 1) < HALF, -sin, sin)
    def turned(t):
        t = t.astype(BF16).astype(F32)
        return (t * cos_s[...] + pltpu.roll(t, HALF, 1) * sin_s[...]).astype(BF16)

    def project(t, count):
        for n in range(count):
            with jax.named_scope("w_wait"):
                wait_tile(t + n)
        return [_dot(a[...], wt[(t + n) % SLOTS], 1, 0) for n in range(count)]

    def refill(t, count):
        for n in range(count):
            start_tile(jnp.int32(t + n + SLOTS))

    def kv_copy(i, rows=pl.ds(0, 2 * ROWS)):
        return remote(kv_out.at[i, rows], kv.at[me, rows], kv_ss.at[0], kv_rs.at[_batch(i, KV_BATCH)], 2 * other(_pick(i, OUT)) + core)

    def q_copy(h, i):
        return remote(q_out.at[h, i], qs.at[h, chip], q_ss.at[0], q_rs.at[_batch(i, Q_BATCH) if isinstance(h, int) and h == 0 else 3 + h], 2 * other(_pick(i, OUT)) + core)

    def keep_k(i, r):
        kv_out[i, :ROWS, :] = turned(r)

    def keep_v(i, r):
        v = r.astype(BF16).T
        kv_out[i, ROWS : ROWS + HEAD, :] = v[:, :HEAD]
        kv_out[i, ROWS + HEAD :, :] = v[:, HEAD:]

    def keep_q(h, i, r):
        q_out[h, i] = turned(r[:, :HEAD])
        q_out[h, i + 1] = turned(r[:, HEAD:])

    def project_first(n, _):
        *rs, r = project(3 * n, 3)
        for i, kv_r in zip((2 * n, 2 * n + 1), rs):
            keep_k(i, kv_r[:, :HEAD])
            keep_v(i, kv_r[:, HEAD:])
        keep_q(0, 2 * n, r)
        refill(3 * n, 3)
        kv_copy(2 * n).start()

        @pl.when(n < CHIPS // 2 - 1)
        def _():
            kv_copy(2 * n + 1).start()

        q_copy(0, 2 * n).start()

        @pl.when(n < CHIPS // 2 - 1)
        def _():
            q_copy(0, 2 * n + 1).start()

        return _

    with jax.named_scope("project_0"):
        r = project(0, 1)[0]
        for i in range(2):
            keep_k(i, r[:, i * HEAD : (i + 1) * HEAD])
        with jax.named_scope("barrier"):
            pl.semaphore_wait(barrier, CHIPS)
        for i in range(2):
            kv_copy(i, pl.ds(0, ROWS)).start()
        r = project(1, 1)[0]
        for i in range(2):
            keep_v(i, r[:, i * HEAD : (i + 1) * HEAD])
            kv_copy(i, pl.ds(ROWS, ROWS)).start()
        keep_q(0, 0, project(2, 1)[0])
        for i in range(2):
            q_copy(0, i).start()
        refill(0, 3)
    with jax.named_scope("project_first"):
        lax.fori_loop(1, CHIPS // 2, project_first, None)
    own_kv = pltpu.make_async_copy(kv_out.at[CHIPS - 1], kv.at[me], own_sem)
    own_kv.start()

    def relay(p):
        b = 2 * other(IN[p]) + core
        return remote(kv.at[b], kv.at[b], rl_ss.at[0], kv_rs.at[2 + p // 2], sibling)

    def pass_on(batch):
        received(kv.at[pl.ds(0, KV_BATCH[:-1].count(batch))], kv_rs.at[batch])
        for p in ((1, 2, 3, 4, 5), (6, 7))[batch]:
            relay(p).start()

    def project_q(n, _):
        t = 2 * n + 3 * CHIPS // 2
        rs = project(t, 2)
        h, i0 = 1 + n // 2, 4 * (n % 2)
        for m, r in enumerate(rs):
            q_out[h, i0 + 2 * m] = turned(r[:, :HEAD])
            q_out[h, i0 + 2 * m + 1] = turned(r[:, HEAD:])
        refill(t, 2)
        for m in range(4):
            early = [[i for i in range(CHIPS - 1) if i not in late] for late in LATE]
            for first in (0, 4):
                hs = [h_ for h_ in (1, 2) if first + m in early[h_ - 1]]
                if hs:
                    @pl.when((i0 == first) & ((h == hs[0]) | (h == hs[-1])))
                    def _():
                        q_copy(h, first + m).start()

        return _

    with jax.named_scope("project_q"):
        own_kv.wait()
        relay(0).start()
        lax.fori_loop(0, CHIPS // 2, project_q, None)
        own_q = [pltpu.make_async_copy(q_out.at[h, CHIPS - 1], qs.at[h, chip], ownq_sem) for h in range(GROUP)]
        begin(own_q)
    with jax.named_scope("pass_on"):
        pass_on(0)

    def wo_copy(h, g):
        return pltpu.make_async_copy(wo.at[pl.ds((GROUP * g + h) * HEAD, HEAD), :], wos.at[h, pl.ds(g * HEAD, HEAD), :], wo_sem.at[h])

    for h in range(GROUP):
        for g in range(CHIPS):
            wo_copy(h, g).start()
    done(qs.at[pl.ds(0, GROUP), 0], ownq_sem)

    def arrive(n):
        received(kv.at[pl.ds(0, 2)], kv_rs.at[2 + n])

        @pl.when(n == 0)
        def _():
            received(qs.at[0, pl.ds(0, 1)], q_rs.at[0])

        @pl.when(n > 0)
        def _():
            received(qs.at[0, pl.ds(0, 2)], q_rs.at[n])

    def at(sq, sk):
        return sq * (sq + 1) // 2 + sk

    ones = jnp.ones((8, 2 * ROWS), BF16)

    def attend(h, items):
        def score(sq, sk, masked, _):
            k = jnp.concatenate([kv[2 * sk, :ROWS, :], kv[2 * sk + 1, :ROWS, :]], axis=0)
            s = _dot(k, qs[h, sq], 1, 1)
            if masked:
                gap = lax.broadcasted_iota(jnp.int32, s.shape, 1) - lax.broadcasted_iota(jnp.int32, s.shape, 0)
                s = jnp.where(gap >= -ROWS * core, s, HIDDEN)
            return s

        def weigh(s, to):
            top = s.max(axis=0, keepdims=True)
            tops[to] = jnp.broadcast_to(top, (8, ROWS))
            return jnp.exp2((s - top) * E).astype(BF16)

        def add_up(p, sk, to):
            v = jnp.concatenate([kv[2 * sk + c, ROWS + n * HEAD : ROWS + (n + 1) * HEAD, :] for c in range(2) for n in range(2)], axis=1)
            part[to] = _dot(jnp.concatenate([v, ones], axis=0), p, 1, 0)

        s, p = {}, {}
        for n in range(len(items) + LAG_P):
            if n < len(items):
                s[n] = score(*items[n])
            if 0 <= n - LAG_W < len(items):
                m = n - LAG_W
                p[m] = weigh(s.pop(m), items[m][3])
            if 0 <= n - LAG_P < len(items):
                m = n - LAG_P
                add_up(p.pop(m), items[m][1], items[m][3])

    def o_copy(h, i):
        sq = other(_pick(i, OUT))
        return remote(o_out.at[h, sq], os.at[h, chip], o_ss.at[0], o_rs.at[_late(h, i)], 2 * sq + core)

    def pair(s0, s1):
        sq, sk = jnp.maximum(s0, s1), jnp.minimum(s0, s1)
        return sq, sk, False, at(sq, sk)

    def first_head(n, _):
        with jax.named_scope("arrive"):
            arrive(n)
        s0, s1 = other(_pick(2 * n, IN)), other(_pick(2 * n + 1, IN))
        attend(0, [(s0, s0, True, at(s0, s0)), (s1, s1, True, at(s1, s1)), pair(s0, s1)])

        def earlier(m, _):
            s2, s3 = other(_pick(2 * m, IN)), other(_pick(2 * m + 1, IN))
            attend(0, [pair(s, t) for t in (s2, s3) for s in (s0, s1)])
            return _

        with jax.named_scope("earlier"):
            lax.fori_loop(0, n, earlier, None)

        @pl.when(n == 1)
        def _():
            with jax.named_scope("pass_on"):
                pass_on(1)

        @pl.when(n == 0)
        def _():
            for h, late in enumerate(LATE, 1):
                for i in late:
                    q_copy(h, i).start()

        return _

    def finish(h, sq, slots, shown=None):
        t = [tops[n] for n in slots]
        if shown is not None:
            t = [jnp.where(show, x, HIDDEN) for show, x in zip(shown, t)]
        top = functools.reduce(jnp.maximum, t)
        acc = sum(part[n] * jnp.exp2((x - top) * E)[:1] for n, x in zip(slots, t))
        o_out[h, sq] = (acc[:HEAD] * (1 / acc[HEAD : HEAD + 1])).T.astype(BF16)

    with jax.named_scope("head_0"):
        lax.fori_loop(0, CHIPS // 2, first_head, None)
    with jax.named_scope("finish"):
        for sq in range(CHIPS):
            finish(0, sq, [at(sq, n) for n in range(sq + 1)])
        for i in range(CHIPS - 1):
            o_copy(0, i).start()

    def later_head(h, _):
        with jax.named_scope("q_wait"):
            received(qs.at[h, pl.ds(0, CHIPS - 1)], q_rs.at[3 + h])

        def two(r, _):
            s0 = other(_pick(2 * r, OUT))
            big, small = jnp.maximum(s0, CHIPS - 1 - s0), jnp.minimum(s0, CHIPS - 1 - s0)
            items = [(big, big, True, 0), (small, small, True, 1)]
            for j in range(CHIPS - 1):
                items.append((jnp.where(j < big, big, small), jnp.where(j < big, j, j - big), False, j + 2))
            for n in range(0, len(items), STEP):
                attend(h, items[n : n + STEP])
            finish(h, big, (0, *range(2, 9)), [True, *(j < big for j in range(CHIPS - 1))])
            finish(h, small, (1, *range(2, 9)), [True, *(j >= big for j in range(CHIPS - 1))])
            o_copy(h, 2 * r).start()

            @pl.when(r < CHIPS // 2 - 1)
            def _():
                o_copy(h, 2 * r + 1).start()

            return _

        with jax.named_scope("rounds"):
            lax.fori_loop(0, CHIPS // 2, two, None)
        return _

    lax.fori_loop(1, GROUP, later_head, None)

    def columns(parts, first, last):
        def body(n, _):
            cols = pl.ds(pl.multiple_of(n * COLS, COLS), COLS)
            seen = jnp.concatenate([os[h, g] for h, g in parts], axis=1)
            w = jnp.concatenate([wos[h, pl.ds(pl.multiple_of(g * HEAD, HEAD), HEAD), cols] for h, g in parts], axis=0)
            r = _dot(seen, w, 1, 0)
            r += xs[:, cols].astype(F32) if first else yacc[:, cols]
            if last:
                y_ref[:, cols] = r.astype(BF16)
            else:
                yacc[:, cols] = r
            return _

        with jax.named_scope("columns"):
            lax.fori_loop(0, D // COLS, body, None)

    own_o = [pltpu.make_async_copy(o_out.at[h, chip], os.at[h, chip], ownq_sem) for h in range(GROUP)]
    begin(own_o)
    done(os.at[pl.ds(0, GROUP), 0], ownq_sem)
    with jax.named_scope("wo_wait"):
        for h in range(GROUP):
            pltpu.make_async_copy(wo.at[pl.ds(0, CHIPS * HEAD), :], wos.at[h], wo_sem.at[h]).wait()
    with jax.named_scope("o_wait"):
        received(os.at[0, pl.ds(0, CHIPS - 1)], o_rs.at[0])
    columns([(0, g) for g in range(CHIPS)], True, False)
    with jax.named_scope("o_wait"):
        received(os.at[1, pl.ds(0, CHIPS - 1)], o_rs.at[1])
    columns([(1, g) for g in range(CHIPS)], False, False)
    for n, (p0, p1) in enumerate(zip(PARTS, PARTS[1:])):
        with jax.named_scope("o_wait"):
            received(os.at[2, pl.ds(0, min(p1, CHIPS - 1) - p0)], o_rs.at[2 + n])
        columns([(2, other(m)) for m in OUT[p0:p1]], False, p1 == CHIPS)

    with jax.named_scope("sent"):
        sent(kv.at[pl.ds(0, CHIPS)], rl_ss.at[0])
        sent(kv_out.at[pl.ds(0, CHIPS - 1)], kv_ss.at[0])
        sent(q_out.at[pl.ds(0, GROUP), pl.ds(0, CHIPS - 1)], q_ss.at[0])
        sent(o_out.at[pl.ds(0, GROUP), pl.ds(0, CHIPS - 1)], o_ss.at[0])


def _tables():
    rate = float(THETA) ** (-np.arange(HALF) / HALF)
    def both(place):
        angle = np.tile(place[:, None] * rate, 2)
        return np.stack([np.cos(angle), np.sin(angle)]).astype(np.float32)
    return both(np.arange(ROWS, dtype=np.float64)), both(ROWS * np.arange(2 * CHIPS, dtype=np.float64))


def solution(mesh):
    rot, off = _tables()
    dma = pltpu.SemaphoreType.DMA
    anywhere, vmem = pl.BlockSpec(memory_space=pl.ANY), pl.BlockSpec(memory_space=pltpu.VMEM)

    def step(x, gain, wq, wk, wv, wo):
        block = (ROWS, HEAD)
        return pl.pallas_call(
            _kernel,
            out_shape=pltpu.VMEM((ROWS, D), BF16),
            in_specs=[anywhere] * 8,
            out_specs=vmem,
            scratch_shapes=[
                pltpu.VMEM((ROWS, D), BF16),
                pltpu.VMEM((D,), BF16),
                pltpu.VMEM((2, *block), F32),
                pltpu.VMEM((2, 2 * CHIPS, HEAD), F32),
                pltpu.VMEM((ROWS, D), BF16),
                pltpu.VMEM(block, F32),
                pltpu.VMEM(block, F32),
                pltpu.VMEM((SLOTS, D, 2 * HEAD), BF16),
                pltpu.VMEM((GROUP, CHIPS * HEAD, D), BF16),
                pltpu.VMEM((CHIPS, 2 * ROWS, HEAD), BF16),
                pltpu.VMEM((2 * CHIPS, 2 * ROWS, HEAD), BF16),
                pltpu.VMEM((GROUP, CHIPS, *block), BF16),
                pltpu.VMEM((GROUP, CHIPS, *block), BF16),
                pltpu.VMEM((GROUP, CHIPS, *block), BF16),
                pltpu.VMEM((GROUP, CHIPS, *block), BF16),
                pltpu.VMEM((CHIPS * (CHIPS + 1) // 2, HEAD + 8, ROWS), F32),
                pltpu.VMEM((CHIPS * (CHIPS + 1) // 2, 8, ROWS), F32),
                pltpu.VMEM((ROWS, D), F32),
                dma((X_PARTS,)),
                dma((3,)),
                dma,
                dma,
                dma((SLOTS,)),
                dma((GROUP,)),
                dma((1,)),
                dma((2 + CHIPS // 2,)),
                dma((1,)),
                dma((1,)),
                dma((CHIPS // 2 + GROUP - 1,)),
                dma((1,)),
                dma((GROUP + len(PARTS) - 2,)),
            ],
            compiler_params=pltpu.CompilerParams(collective_id=0, has_side_effects=True, vmem_limit_bytes=62 * 2**20),
        )(x, gain, jnp.asarray(rot), jnp.asarray(off), wq, wk, wv, wo)

    tokens, whole = P(("dp", "sp"), None), P(None, None)
    return jax.shard_map(
        step,
        mesh=mesh,
        in_specs=(tokens, P(None), whole, whole, whole, whole),
        out_specs=tokens,
        check_vma=False,
    )
```

```python
import functools

import jax
import jax.numpy as jnp
import numpy as np
from jax import lax
from jax.experimental import pallas as pl
from jax.experimental.pallas import tpu as pltpu
from jax.sharding import PartitionSpec as P

HEAD = 128
HALF = HEAD // 2
THETA = 10000
CHIPS = 8
GROUP = 3
ROWS = 256
D = 3072
HIDDEN = -3e38
E = HEAD**-0.5 * 1.4426950408889634
OUT = (6, 1, 5, 2, 3, 4, 7, 0)
IN = (0, 6, 1, 5, 2, 3, 4, 7)
LATE = ((1, 3, 4), (1, 3, 4))
PARTS = (0, 4, 6, 8)
SLOTS = 6
KV_TILES, Q_TILES = CHIPS, CHIPS * GROUP // 2
TILES = KV_TILES + Q_TILES
COLS = 1536
LAST_COLS = 3072
X_PARTS = 4
STEP = 9
LAG_W, LAG_P = 3, 5
F32, BF16 = jnp.float32, jnp.bfloat16


def _dot(a, b, ca, cb):
    return lax.dot_general(a, b, (((ca,), (cb,)), ((), ())), preferred_element_type=F32)


def _pick(i, table):
    r = jnp.int32(table[0])
    for n, v in enumerate(table[1:], 1):
        r = jnp.where(i == n, jnp.int32(v), r)
    return r


KV_BATCH = (0, 0, 0, 0, 0, 1, 1, 1)
Q_BATCH = (0, 1, 1, 2, 2, 3, 3, 0)


def _batch(i, table):
    return table[i] if isinstance(i, int) else _pick(i, table)


def _late(h, i):
    return jnp.where(h == GROUP - 1, h + sum(jnp.where(i >= p, 1, 0) for p in PARTS[1:-1]), h)


def _kernel(x_hbm, gain_hbm, rot_hbm, off_hbm, wq, wk, wv, wo, y_ref, xs, gain_ref, rot_ref, off_ref, a, cos_s, sin_s, wt, wos, kv_out, kv, q_out, qs, o_out, os, part, tops, yacc,
            x_sem, table_sem, own_sem, ownq_sem, w_sem, wo_sem, kv_ss, kv_rs, rl_ss, q_ss, q_rs, o_ss, o_rs):
    me = lax.axis_index("sp")
    chip, core = me // 2, me % 2
    sibling = 2 * chip + 1 - core

    def other(mask):
        return jnp.bitwise_xor(chip, mask)

    def remote(src, dst, ss, rs, dev):
        return pltpu.make_async_remote_copy(src_ref=src, dst_ref=dst, send_sem=ss, recv_sem=rs, device_id={"sp": dev}, device_id_type=pl.DeviceIdType.MESH)

    def received(dst, sem):
        remote(dst, dst, sem, sem, sibling).wait_recv()

    def sent(src, sem):
        remote(src, src, sem, sem, sibling).wait_send()

    def done(ref, sem):
        pltpu.make_async_copy(ref, ref, sem).wait()

    def x_copy(i):
        rows = pl.ds(i * (ROWS // X_PARTS), ROWS // X_PARTS)
        return pltpu.make_async_copy(x_hbm.at[rows], xs.at[rows], x_sem.at[i])

    gain_copy, rot_copy, off_copy = (pltpu.make_async_copy(src, dst, table_sem.at[n]) for n, (src, dst) in enumerate(
        ((gain_hbm, gain_ref), (rot_hbm, rot_ref), (off_hbm, off_ref))))
    gain_copy.start()
    for i in range(X_PARTS):
        x_copy(i).start()
    rot_copy.start()
    off_copy.start()

    def halves(slot, w0, at0, w1, at1):
        at0, at1 = pl.multiple_of(at0 * HEAD, HEAD), pl.multiple_of(at1 * HEAD, HEAD)
        return [pltpu.make_async_copy(w0.at[:, pl.ds(at0, HEAD)], wt.at[slot, :, pl.ds(0, HEAD)], w_sem.at[slot]),
                pltpu.make_async_copy(w1.at[:, pl.ds(at1, HEAD)], wt.at[slot, :, pl.ds(HEAD, HEAD)], w_sem.at[slot])]

    def kv_tile(slot, i):
        d = other(_pick(i, OUT))
        return halves(slot, wk, d, wv, d)

    def q_tile(slot, h, pair):
        d0, d1 = other(_pick(2 * pair, OUT)), other(_pick(2 * pair + 1, OUT))
        return halves(slot, wq, GROUP * d0 + h, wq, GROUP * d1 + h)

    def begin(copies):
        for c in copies:
            c.start()

    def start_tile(t):
        slot, first = t % SLOTS, t < 3 * CHIPS // 2

        @pl.when(first & (t % 3 < 2))
        def _():
            begin(kv_tile(slot, 2 * (t // 3) + t % 3))

        @pl.when(first & (t % 3 == 2))
        def _():
            begin(q_tile(slot, 0, t // 3))

        @pl.when((t >= 3 * CHIPS // 2) & (t < TILES))
        def _():
            j = t - 3 * CHIPS // 2
            begin(q_tile(slot, 1 + j // 4, j % 4))

    def wait_tile(t):
        done(wt.at[t % SLOTS], w_sem.at[t % SLOTS])

    barrier = pltpu.get_barrier_semaphore()
    for m in range(1, CHIPS):
        pl.semaphore_signal(barrier, inc=1, device_id={"sp": 2 * other(m) + core}, device_id_type=pl.DeviceIdType.MESH)
    pl.semaphore_signal(barrier, inc=1, device_id={"sp": sibling}, device_id_type=pl.DeviceIdType.MESH)

    d0, d1 = other(OUT[0]), other(OUT[1])
    begin(halves(0, wk, d0, wk, d1))
    with jax.named_scope("norm"):
        gain_copy.wait()
        gain = gain_ref[...].reshape(1, D).astype(F32)
        for i in range(X_PARTS):
            x_copy(i).wait()
            if i == 0:
                begin(halves(1, wv, d0, wv, d1))
                begin(q_tile(2, 0, 0))
            rows = pl.ds(i * (ROWS // X_PARTS), ROWS // X_PARTS)
            wide = xs[rows, :].astype(F32)
            scale = lax.rsqrt(jnp.mean(wide * wide, -1, keepdims=True) + 1e-6)
            a[rows, :] = (wide * scale * gain).astype(BF16)
        begin(kv_tile(3, 2))
        begin(kv_tile(4, 3))
        begin(q_tile(5, 0, 1))

    with jax.named_scope("tables"):
        rot_copy.wait()
        off_copy.wait()
        c0, s0 = off_ref[0, pl.ds(me, 1), :], off_ref[1, pl.ds(me, 1), :]
        cos_s[...] = c0 * rot_ref[0] - s0 * rot_ref[1]
        sin = s0 * rot_ref[0] + c0 * rot_ref[1]
        sin_s[...] = jnp.where(lax.broadcasted_iota(jnp.int32, sin.shape, 1) < HALF, -sin, sin)
    def turned(t):
        t = t.astype(BF16).astype(F32)
        return (t * cos_s[...] + pltpu.roll(t, HALF, 1) * sin_s[...]).astype(BF16)

    def project(t, count):
        for n in range(count):
            with jax.named_scope("w_wait"):
                wait_tile(t + n)
        return [_dot(a[...], wt[(t + n) % SLOTS], 1, 0) for n in range(count)]

    def refill(t, count):
        for n in range(count):
            start_tile(jnp.int32(t + n + SLOTS))

    def kv_copy(i, rows=pl.ds(0, 2 * ROWS)):
        return remote(kv_out.at[i, rows], kv.at[me, rows], kv_ss.at[0], kv_rs.at[_batch(i, KV_BATCH)], 2 * other(_pick(i, OUT)) + core)

    def q_copy(h, i):
        return remote(q_out.at[h, i], qs.at[h, chip], q_ss.at[0], q_rs.at[_batch(i, Q_BATCH) if isinstance(h, int) and h == 0 else 3 + h], 2 * other(_pick(i, OUT)) + core)

    def keep_k(i, r):
        kv_out[i, :ROWS, :] = turned(r)

    def keep_v(i, r):
        v = r.astype(BF16).T
        kv_out[i, ROWS : ROWS + HEAD, :] = v[:, :HEAD]
        kv_out[i, ROWS + HEAD :, :] = v[:, HEAD:]

    def keep_q(h, i, r):
        q_out[h, i] = turned(r[:, :HEAD])
        q_out[h, i + 1] = turned(r[:, HEAD:])

    def project_first(n, _):
        *rs, r = project(3 * n, 3)
        for i, kv_r in zip((2 * n, 2 * n + 1), rs):
            keep_k(i, kv_r[:, :HEAD])
            keep_v(i, kv_r[:, HEAD:])
        keep_q(0, 2 * n, r)
        refill(3 * n, 3)
        kv_copy(2 * n).start()

        @pl.when(n < CHIPS // 2 - 1)
        def _():
            kv_copy(2 * n + 1).start()

        q_copy(0, 2 * n).start()

        @pl.when(n < CHIPS // 2 - 1)
        def _():
            q_copy(0, 2 * n + 1).start()

        return _

    with jax.named_scope("project_0"):
        r = project(0, 1)[0]
        for i in range(2):
            keep_k(i, r[:, i * HEAD : (i + 1) * HEAD])
        with jax.named_scope("barrier"):
            pl.semaphore_wait(barrier, CHIPS)
        for i in range(2):
            kv_copy(i, pl.ds(0, ROWS)).start()
        r = project(1, 1)[0]
        for i in range(2):
            keep_v(i, r[:, i * HEAD : (i + 1) * HEAD])
            kv_copy(i, pl.ds(ROWS, ROWS)).start()
        keep_q(0, 0, project(2, 1)[0])
        for i in range(2):
            q_copy(0, i).start()
        refill(0, 3)
    with jax.named_scope("project_first"):
        lax.fori_loop(1, CHIPS // 2, project_first, None)
    own_kv = pltpu.make_async_copy(kv_out.at[CHIPS - 1], kv.at[me], own_sem)
    own_kv.start()

    def relay(p):
        b = 2 * other(IN[p]) + core
        return remote(kv.at[b], kv.at[b], rl_ss.at[0], kv_rs.at[2 + p // 2], sibling)

    def pass_on(batch):
        received(kv.at[pl.ds(0, KV_BATCH[:-1].count(batch))], kv_rs.at[batch])
        for p in ((1, 2, 3, 4, 5), (6, 7))[batch]:
            relay(p).start()

    def project_q(n, _):
        t = 2 * n + 3 * CHIPS // 2
        rs = project(t, 2)
        h, i0 = 1 + n // 2, 4 * (n % 2)
        for m, r in enumerate(rs):
            q_out[h, i0 + 2 * m] = turned(r[:, :HEAD])
            q_out[h, i0 + 2 * m + 1] = turned(r[:, HEAD:])
        refill(t, 2)
        for m in range(4):
            early = [[i for i in range(CHIPS - 1) if i not in late] for late in LATE]
            for first in (0, 4):
                hs = [h_ for h_ in (1, 2) if first + m in early[h_ - 1]]
                if hs:
                    @pl.when((i0 == first) & ((h == hs[0]) | (h == hs[-1])))
                    def _():
                        q_copy(h, first + m).start()

        return _

    with jax.named_scope("project_q"):
        own_kv.wait()
        relay(0).start()
        lax.fori_loop(0, CHIPS // 2, project_q, None)
        own_q = [pltpu.make_async_copy(q_out.at[h, CHIPS - 1], qs.at[h, chip], ownq_sem) for h in range(GROUP)]
        begin(own_q)
    with jax.named_scope("pass_on"):
        pass_on(0)

    def wo_copy(h, g):
        return pltpu.make_async_copy(wo.at[pl.ds((GROUP * g + h) * HEAD, HEAD), :], wos.at[h, pl.ds(g * HEAD, HEAD), :], wo_sem.at[h])

    for h in range(GROUP):
        for g in range(CHIPS):
            wo_copy(h, g).start()
    done(qs.at[pl.ds(0, GROUP), 0], ownq_sem)

    def arrive(n):
        received(kv.at[pl.ds(0, 2)], kv_rs.at[2 + n])

        @pl.when(n == 0)
        def _():
            received(qs.at[0, pl.ds(0, 1)], q_rs.at[0])

        @pl.when(n > 0)
        def _():
            received(qs.at[0, pl.ds(0, 2)], q_rs.at[n])

    def at(sq, sk):
        return sq * (sq + 1) // 2 + sk

    ones = jnp.ones((8, 2 * ROWS), BF16)

    def attend(h, items):
        def score(sq, sk, masked, _):
            k = jnp.concatenate([kv[2 * sk, :ROWS, :], kv[2 * sk + 1, :ROWS, :]], axis=0)
            s = _dot(k, qs[h, sq], 1, 1)
            if masked:
                gap = lax.broadcasted_iota(jnp.int32, s.shape, 1) - lax.broadcasted_iota(jnp.int32, s.shape, 0)
                s = jnp.where(gap >= -ROWS * core, s, HIDDEN)
            return s

        def weigh(s, to):
            top = s.max(axis=0, keepdims=True)
            tops[to] = jnp.broadcast_to(top, (8, ROWS))
            return jnp.exp2((s - top) * E).astype(BF16)

        def add_up(p, sk, to):
            v = jnp.concatenate([kv[2 * sk + c, ROWS + n * HEAD : ROWS + (n + 1) * HEAD, :] for c in range(2) for n in range(2)], axis=1)
            part[to] = _dot(jnp.concatenate([v, ones], axis=0), p, 1, 0)

        s, p = {}, {}
        for n in range(len(items) + LAG_P):
            if n < len(items):
                s[n] = score(*items[n])
            if 0 <= n - LAG_W < len(items):
                m = n - LAG_W
                p[m] = weigh(s.pop(m), items[m][3])
            if 0 <= n - LAG_P < len(items):
                m = n - LAG_P
                add_up(p.pop(m), items[m][1], items[m][3])

    def o_copy(h, i):
        sq = other(_pick(i, OUT))
        return remote(o_out.at[h, sq], os.at[h, chip], o_ss.at[0], o_rs.at[_late(h, i)], 2 * sq + core)

    def pair(s0, s1):
        sq, sk = jnp.maximum(s0, s1), jnp.minimum(s0, s1)
        return sq, sk, False, at(sq, sk)

    def first_head(n, _):
        with jax.named_scope("arrive"):
            arrive(n)
        s0, s1 = other(_pick(2 * n, IN)), other(_pick(2 * n + 1, IN))
        attend(0, [(s0, s0, True, at(s0, s0)), (s1, s1, True, at(s1, s1)), pair(s0, s1)])

        def earlier(m, _):
            s2, s3 = other(_pick(2 * m, IN)), other(_pick(2 * m + 1, IN))
            attend(0, [pair(s, t) for t in (s2, s3) for s in (s0, s1)])
            return _

        with jax.named_scope("earlier"):
            lax.fori_loop(0, n, earlier, None)

        @pl.when(n == 1)
        def _():
            with jax.named_scope("pass_on"):
                pass_on(1)

        @pl.when(n == 0)
        def _():
            for h, late in enumerate(LATE, 1):
                for i in late:
                    q_copy(h, i).start()

        return _

    def finish(h, sq, slots, shown=None):
        t = [tops[n] for n in slots]
        if shown is not None:
            t = [jnp.where(show, x, HIDDEN) for show, x in zip(shown, t)]
        top = functools.reduce(jnp.maximum, t)
        acc = sum(part[n] * jnp.exp2((x - top) * E)[:1] for n, x in zip(slots, t))
        o_out[h, sq] = (acc[:HEAD] * (1 / acc[HEAD : HEAD + 1])).T.astype(BF16)

    with jax.named_scope("head_0"):
        lax.fori_loop(0, CHIPS // 2, first_head, None)
    with jax.named_scope("finish"):
        for sq in range(CHIPS):
            finish(0, sq, [at(sq, n) for n in range(sq + 1)])
        for i in range(CHIPS - 1):
            o_copy(0, i).start()

    def later_head(h, _):
        with jax.named_scope("q_wait"):
            received(qs.at[h, pl.ds(0, CHIPS - 1)], q_rs.at[3 + h])

        def two(r, _):
            s0 = other(_pick(2 * r, OUT))
            big, small = jnp.maximum(s0, CHIPS - 1 - s0), jnp.minimum(s0, CHIPS - 1 - s0)
            items = [(big, big, True, 0), (small, small, True, 1)]
            for j in range(CHIPS - 1):
                items.append((jnp.where(j < big, big, small), jnp.where(j < big, j, j - big), False, j + 2))
            for n in range(0, len(items), STEP):
                attend(h, items[n : n + STEP])
            finish(h, big, (0, *range(2, 9)), [True, *(j < big for j in range(CHIPS - 1))])
            finish(h, small, (1, *range(2, 9)), [True, *(j >= big for j in range(CHIPS - 1))])
            o_copy(h, 2 * r).start()

            @pl.when(r < CHIPS // 2 - 1)
            def _():
                o_copy(h, 2 * r + 1).start()

            return _

        with jax.named_scope("rounds"):
            lax.fori_loop(0, CHIPS // 2, two, None)
        return _

    lax.fori_loop(1, GROUP, later_head, None)

    def columns(parts, first, last):
        width = LAST_COLS if last else COLS

        def body(n, _):
            cols = pl.ds(pl.multiple_of(n * width, width), width)
            seen = jnp.concatenate([os[h, g] for h, g in parts], axis=1)
            w = jnp.concatenate([wos[h, pl.ds(pl.multiple_of(g * HEAD, HEAD), HEAD), cols] for h, g in parts], axis=0)
            r = _dot(seen, w, 1, 0)
            r += xs[:, cols].astype(F32) if first else yacc[:, cols]
            if last:
                y_ref[:, cols] = r.astype(BF16)
            else:
                yacc[:, cols] = r
            return _

        with jax.named_scope("columns"):
            lax.fori_loop(0, D // width, body, None)

    own_o = [pltpu.make_async_copy(o_out.at[h, chip], os.at[h, chip], ownq_sem) for h in range(GROUP)]
    begin(own_o)
    done(os.at[pl.ds(0, GROUP), 0], ownq_sem)
    with jax.named_scope("wo_wait"):
        for h in range(GROUP):
            pltpu.make_async_copy(wo.at[pl.ds(0, CHIPS * HEAD), :], wos.at[h], wo_sem.at[h]).wait()
    with jax.named_scope("o_wait"):
        received(os.at[0, pl.ds(0, CHIPS - 1)], o_rs.at[0])
    columns([(0, g) for g in range(CHIPS)], True, False)
    with jax.named_scope("o_wait"):
        received(os.at[1, pl.ds(0, CHIPS - 1)], o_rs.at[1])
    columns([(1, g) for g in range(CHIPS)], False, False)
    for n, (p0, p1) in enumerate(zip(PARTS, PARTS[1:])):
        with jax.named_scope("o_wait"):
            received(os.at[2, pl.ds(0, min(p1, CHIPS - 1) - p0)], o_rs.at[2 + n])
        columns([(2, other(m)) for m in OUT[p0:p1]], False, p1 == CHIPS)

    with jax.named_scope("sent"):
        sent(kv.at[pl.ds(0, CHIPS)], rl_ss.at[0])
        sent(kv_out.at[pl.ds(0, CHIPS - 1)], kv_ss.at[0])
        sent(q_out.at[pl.ds(0, GROUP), pl.ds(0, CHIPS - 1)], q_ss.at[0])
        sent(o_out.at[pl.ds(0, GROUP), pl.ds(0, CHIPS - 1)], o_ss.at[0])


def _tables():
    rate = float(THETA) ** (-np.arange(HALF) / HALF)
    def both(place):
        angle = np.tile(place[:, None] * rate, 2)
        return np.stack([np.cos(angle), np.sin(angle)]).astype(np.float32)
    return both(np.arange(ROWS, dtype=np.float64)), both(ROWS * np.arange(2 * CHIPS, dtype=np.float64))


def solution(mesh):
    rot, off = _tables()
    dma = pltpu.SemaphoreType.DMA
    anywhere, vmem = pl.BlockSpec(memory_space=pl.ANY), pl.BlockSpec(memory_space=pltpu.VMEM)

    def step(x, gain, wq, wk, wv, wo):
        block = (ROWS, HEAD)
        return pl.pallas_call(
            _kernel,
            out_shape=pltpu.VMEM((ROWS, D), BF16),
            in_specs=[anywhere] * 8,
            out_specs=vmem,
            scratch_shapes=[
                pltpu.VMEM((ROWS, D), BF16),
                pltpu.VMEM((D,), BF16),
                pltpu.VMEM((2, *block), F32),
                pltpu.VMEM((2, 2 * CHIPS, HEAD), F32),
                pltpu.VMEM((ROWS, D), BF16),
                pltpu.VMEM(block, F32),
                pltpu.VMEM(block, F32),
                pltpu.VMEM((SLOTS, D, 2 * HEAD), BF16),
                pltpu.VMEM((GROUP, CHIPS * HEAD, D), BF16),
                pltpu.VMEM((CHIPS, 2 * ROWS, HEAD), BF16),
                pltpu.VMEM((2 * CHIPS, 2 * ROWS, HEAD), BF16),
                pltpu.VMEM((GROUP, CHIPS, *block), BF16),
                pltpu.VMEM((GROUP, CHIPS, *block), BF16),
                pltpu.VMEM((GROUP, CHIPS, *block), BF16),
                pltpu.VMEM((GROUP, CHIPS, *block), BF16),
                pltpu.VMEM((CHIPS * (CHIPS + 1) // 2, HEAD + 8, ROWS), F32),
                pltpu.VMEM((CHIPS * (CHIPS + 1) // 2, 8, ROWS), F32),
                pltpu.VMEM((ROWS, D), F32),
                dma((X_PARTS,)),
                dma((3,)),
                dma,
                dma,
                dma((SLOTS,)),
                dma((GROUP,)),
                dma((1,)),
                dma((2 + CHIPS // 2,)),
                dma((1,)),
                dma((1,)),
                dma((CHIPS // 2 + GROUP - 1,)),
                dma((1,)),
                dma((GROUP + len(PARTS) - 2,)),
            ],
            compiler_params=pltpu.CompilerParams(collective_id=0, has_side_effects=True, vmem_limit_bytes=62 * 2**20),
        )(x, gain, jnp.asarray(rot), jnp.asarray(off), wq, wk, wv, wo)

    tokens, whole = P(("dp", "sp"), None), P(None, None)
    return jax.shard_map(
        step,
        mesh=mesh,
        in_specs=(tokens, P(None), whole, whole, whole, whole),
        out_specs=tokens,
        check_vma=False,
    )
```

```python
import functools

import jax
import jax.numpy as jnp
import numpy as np
from jax import lax
from jax.experimental import pallas as pl
from jax.experimental.pallas import tpu as pltpu
from jax.sharding import PartitionSpec as P

HEAD = 128
HALF = HEAD // 2
THETA = 10000
CHIPS = 8
GROUP = 3
ROWS = 256
D = 3072
HIDDEN = -3e38
E = HEAD**-0.5 * 1.4426950408889634
OUT = (6, 1, 5, 2, 3, 4, 7, 0)
IN = (0, 6, 1, 5, 2, 3, 4, 7)
LATE = ((1, 3, 4), (1, 3, 4))
PARTS = (0, 4, 6, 8)
SLOTS = 6
KV_TILES, Q_TILES = CHIPS, CHIPS * GROUP // 2
TILES = KV_TILES + Q_TILES
COLS = 1536
LAST_COLS = 3072
X_PARTS = 4
STEP = 9
LAG_W, LAG_P = 3, 5
F32, BF16 = jnp.float32, jnp.bfloat16


def _dot(a, b, ca, cb):
    return lax.dot_general(a, b, (((ca,), (cb,)), ((), ())), preferred_element_type=F32)


def _pick(i, table):
    r = jnp.int32(table[0])
    for n, v in enumerate(table[1:], 1):
        r = jnp.where(i == n, jnp.int32(v), r)
    return r


KV_BATCH = (0, 0, 0, 0, 0, 1, 1, 1)
Q_BATCH = (0, 1, 1, 2, 2, 3, 3, 0)


def _batch(i, table):
    return table[i] if isinstance(i, int) else _pick(i, table)


def _late(h, i):
    return jnp.where(h == GROUP - 1, h + sum(jnp.where(i >= p, 1, 0) for p in PARTS[1:-1]), h)


def _kernel(x_hbm, gain_hbm, rot_hbm, off_hbm, wq, wk, wv, wo, y_ref, xs, gain_ref, rot_ref, off_ref, a, cos_s, sin_s, wt, wos, kv_out, kv, q_out, qs, o_out, os, part, tops, yacc,
            x_sem, table_sem, own_sem, w_sem, wo_sem, kv_ss, kv_rs, rl_ss, q_ss, q_rs, o_ss, o_rs):
    me = lax.axis_index("sp")
    chip, core = me // 2, me % 2
    sibling = 2 * chip + 1 - core

    def other(mask):
        return jnp.bitwise_xor(chip, mask)

    def remote(src, dst, ss, rs, dev):
        return pltpu.make_async_remote_copy(src_ref=src, dst_ref=dst, send_sem=ss, recv_sem=rs, device_id={"sp": dev}, device_id_type=pl.DeviceIdType.MESH)

    def received(dst, sem):
        remote(dst, dst, sem, sem, sibling).wait_recv()

    def sent(src, sem):
        remote(src, src, sem, sem, sibling).wait_send()

    def done(ref, sem):
        pltpu.make_async_copy(ref, ref, sem).wait()

    def x_copy(i):
        rows = pl.ds(i * (ROWS // X_PARTS), ROWS // X_PARTS)
        return pltpu.make_async_copy(x_hbm.at[rows], xs.at[rows], x_sem.at[i])

    gain_copy, rot_copy, off_copy = (pltpu.make_async_copy(src, dst, table_sem.at[n]) for n, (src, dst) in enumerate(
        ((gain_hbm, gain_ref), (rot_hbm, rot_ref), (off_hbm, off_ref))))
    gain_copy.start()
    for i in range(X_PARTS):
        x_copy(i).start()
    rot_copy.start()
    off_copy.start()

    def halves(slot, w0, at0, w1, at1):
        at0, at1 = pl.multiple_of(at0 * HEAD, HEAD), pl.multiple_of(at1 * HEAD, HEAD)
        return [pltpu.make_async_copy(w0.at[:, pl.ds(at0, HEAD)], wt.at[slot, :, pl.ds(0, HEAD)], w_sem.at[slot]),
                pltpu.make_async_copy(w1.at[:, pl.ds(at1, HEAD)], wt.at[slot, :, pl.ds(HEAD, HEAD)], w_sem.at[slot])]

    def kv_tile(slot, i):
        d = other(_pick(i, OUT))
        return halves(slot, wk, d, wv, d)

    def q_tile(slot, h, pair):
        d0, d1 = other(_pick(2 * pair, OUT)), other(_pick(2 * pair + 1, OUT))
        return halves(slot, wq, GROUP * d0 + h, wq, GROUP * d1 + h)

    def begin(copies):
        for c in copies:
            c.start()

    def start_tile(t):
        slot, first = t % SLOTS, t < 3 * CHIPS // 2

        @pl.when(first & (t % 3 < 2))
        def _():
            begin(kv_tile(slot, 2 * (t // 3) + t % 3))

        @pl.when(first & (t % 3 == 2))
        def _():
            begin(q_tile(slot, 0, t // 3))

        @pl.when((t >= 3 * CHIPS // 2) & (t < TILES))
        def _():
            j = t - 3 * CHIPS // 2
            begin(q_tile(slot, 1 + j // 4, j % 4))

    def wait_tile(t):
        done(wt.at[t % SLOTS], w_sem.at[t % SLOTS])

    barrier = pltpu.get_barrier_semaphore()
    for m in range(1, CHIPS):
        pl.semaphore_signal(barrier, inc=1, device_id={"sp": 2 * other(m) + core}, device_id_type=pl.DeviceIdType.MESH)
    pl.semaphore_signal(barrier, inc=1, device_id={"sp": sibling}, device_id_type=pl.DeviceIdType.MESH)

    d0, d1 = other(OUT[0]), other(OUT[1])
    begin(halves(0, wk, d0, wk, d1))
    with jax.named_scope("norm"):
        gain_copy.wait()
        gain = gain_ref[...].reshape(1, D).astype(F32)
        for i in range(X_PARTS):
            x_copy(i).wait()
            if i == 0:
                begin(halves(1, wv, d0, wv, d1))
                begin(q_tile(2, 0, 0))
            rows = pl.ds(i * (ROWS // X_PARTS), ROWS // X_PARTS)
            wide = xs[rows, :].astype(F32)
            scale = lax.rsqrt(jnp.mean(wide * wide, -1, keepdims=True) + 1e-6)
            a[rows, :] = (wide * scale * gain).astype(BF16)
        begin(kv_tile(3, 2))
        begin(kv_tile(4, 3))
        begin(q_tile(5, 0, 1))

    with jax.named_scope("tables"):
        rot_copy.wait()
        off_copy.wait()
        c0, s0 = off_ref[0, pl.ds(me, 1), :], off_ref[1, pl.ds(me, 1), :]
        cos_s[...] = c0 * rot_ref[0] - s0 * rot_ref[1]
        sin = s0 * rot_ref[0] + c0 * rot_ref[1]
        sin_s[...] = jnp.where(lax.broadcasted_iota(jnp.int32, sin.shape, 1) < HALF, -sin, sin)
    def turned(t):
        t = t.astype(BF16).astype(F32)
        return (t * cos_s[...] + pltpu.roll(t, HALF, 1) * sin_s[...]).astype(BF16)

    def project(t, count):
        for n in range(count):
            with jax.named_scope("w_wait"):
                wait_tile(t + n)
        return [_dot(a[...], wt[(t + n) % SLOTS], 1, 0) for n in range(count)]

    def refill(t, count):
        for n in range(count):
            start_tile(jnp.int32(t + n + SLOTS))

    def kv_copy(i, rows=pl.ds(0, 2 * ROWS)):
        return remote(kv_out.at[i, rows], kv.at[me, rows], kv_ss.at[0], kv_rs.at[_batch(i, KV_BATCH)], 2 * other(_pick(i, OUT)) + core)

    def q_copy(h, i):
        return remote(q_out.at[h, i], qs.at[h, chip], q_ss.at[0], q_rs.at[_batch(i, Q_BATCH) if isinstance(h, int) and h == 0 else 3 + h], 2 * other(_pick(i, OUT)) + core)

    def keep_k(i, r):
        kv_out[i, :ROWS, :] = turned(r)

    def keep_v(i, r):
        v = r.astype(BF16).T
        kv_out[i, ROWS : ROWS + HEAD, :] = v[:, :HEAD]
        kv_out[i, ROWS + HEAD :, :] = v[:, HEAD:]

    def keep_q(h, i, r):
        q_out[h, i] = turned(r[:, :HEAD])
        q_out[h, i + 1] = turned(r[:, HEAD:])

    def project_first(n, _):
        *rs, r = project(3 * n, 3)
        for i, kv_r in zip((2 * n, 2 * n + 1), rs):
            keep_k(i, kv_r[:, :HEAD])
            keep_v(i, kv_r[:, HEAD:])
        keep_q(0, 2 * n, r)
        refill(3 * n, 3)
        kv_copy(2 * n).start()

        @pl.when(n < CHIPS // 2 - 1)
        def _():
            kv_copy(2 * n + 1).start()

        q_copy(0, 2 * n).start()

        @pl.when(n < CHIPS // 2 - 1)
        def _():
            q_copy(0, 2 * n + 1).start()

        return _

    with jax.named_scope("project_0"):
        r = project(0, 1)[0]
        for i in range(2):
            keep_k(i, r[:, i * HEAD : (i + 1) * HEAD])
        with jax.named_scope("barrier"):
            pl.semaphore_wait(barrier, CHIPS)
        for i in range(2):
            kv_copy(i, pl.ds(0, ROWS)).start()
        r = project(1, 1)[0]
        for i in range(2):
            keep_v(i, r[:, i * HEAD : (i + 1) * HEAD])
            kv_copy(i, pl.ds(ROWS, ROWS)).start()
        keep_q(0, 0, project(2, 1)[0])
        for i in range(2):
            q_copy(0, i).start()
        refill(0, 3)
    with jax.named_scope("project_first"):
        lax.fori_loop(1, CHIPS // 2, project_first, None)
    own_kv = pltpu.make_async_copy(kv_out.at[CHIPS - 1], kv.at[me], own_sem)
    own_kv.start()

    def relay(p):
        b = 2 * other(IN[p]) + core
        return remote(kv.at[b], kv.at[b], rl_ss.at[0], kv_rs.at[2 + p // 2], sibling)

    def pass_on(batch):
        received(kv.at[pl.ds(0, KV_BATCH[:-1].count(batch))], kv_rs.at[batch])
        for p in ((1, 2, 3, 4, 5), (6, 7))[batch]:
            relay(p).start()

    def project_q(n, _):
        t = 2 * n + 3 * CHIPS // 2
        rs = project(t, 2)
        h, i0 = 1 + n // 2, 4 * (n % 2)
        for m, r in enumerate(rs):
            q_out[h, i0 + 2 * m] = turned(r[:, :HEAD])
            q_out[h, i0 + 2 * m + 1] = turned(r[:, HEAD:])
        refill(t, 2)
        for m in range(4):
            early = [[i for i in range(CHIPS - 1) if i not in late] for late in LATE]
            for first in (0, 4):
                hs = [h_ for h_ in (1, 2) if first + m in early[h_ - 1]]
                if hs:
                    @pl.when((i0 == first) & ((h == hs[0]) | (h == hs[-1])))
                    def _():
                        q_copy(h, first + m).start()

        return _

    with jax.named_scope("project_q"):
        own_kv.wait()
        relay(0).start()
        lax.fori_loop(0, CHIPS // 2, project_q, None)
        own_q = [pltpu.make_async_copy(q_out.at[h, CHIPS - 1], qs.at[h, chip], own_sem) for h in range(GROUP)]
        begin(own_q)
    with jax.named_scope("pass_on"):
        pass_on(0)

    def wo_copy(h, g):
        return pltpu.make_async_copy(wo.at[pl.ds((GROUP * g + h) * HEAD, HEAD), :], wos.at[h, pl.ds(g * HEAD, HEAD), :], wo_sem)

    for h in range(GROUP):
        for g in range(CHIPS):
            wo_copy(h, g).start()
    done(qs.at[pl.ds(0, GROUP), 0], own_sem)

    def arrive(n):
        received(kv.at[pl.ds(0, 2)], kv_rs.at[2 + n])

        @pl.when(n == 0)
        def _():
            received(qs.at[0, pl.ds(0, 1)], q_rs.at[0])

        @pl.when(n > 0)
        def _():
            received(qs.at[0, pl.ds(0, 2)], q_rs.at[n])

    def at(sq, sk):
        return sq * (sq + 1) // 2 + sk

    ones = jnp.ones((8, 2 * ROWS), BF16)

    def attend(h, items):
        def score(sq, sk, masked, _):
            k = jnp.concatenate([kv[2 * sk, :ROWS, :], kv[2 * sk + 1, :ROWS, :]], axis=0)
            s = _dot(k, qs[h, sq], 1, 1)
            if masked:
                gap = lax.broadcasted_iota(jnp.int32, s.shape, 1) - lax.broadcasted_iota(jnp.int32, s.shape, 0)
                s = jnp.where(gap >= -ROWS * core, s, HIDDEN)
            return s

        def weigh(s, to):
            top = s.max(axis=0, keepdims=True)
            tops[to] = jnp.broadcast_to(top, (8, ROWS))
            return jnp.exp2((s - top) * E).astype(BF16)

        def add_up(p, sk, to):
            v = jnp.concatenate([kv[2 * sk + c, ROWS + n * HEAD : ROWS + (n + 1) * HEAD, :] for c in range(2) for n in range(2)], axis=1)
            part[to] = _dot(jnp.concatenate([v, ones], axis=0), p, 1, 0)

        s, p = {}, {}
        for n in range(len(items) + LAG_P):
            if n < len(items):
                s[n] = score(*items[n])
            if 0 <= n - LAG_W < len(items):
                m = n - LAG_W
                p[m] = weigh(s.pop(m), items[m][3])
            if 0 <= n - LAG_P < len(items):
                m = n - LAG_P
                add_up(p.pop(m), items[m][1], items[m][3])

    def o_copy(h, i):
        sq = other(_pick(i, OUT))
        return remote(o_out.at[h, sq], os.at[h, chip], o_ss.at[0], o_rs.at[_late(h, i)], 2 * sq + core)

    def pair(s0, s1):
        sq, sk = jnp.maximum(s0, s1), jnp.minimum(s0, s1)
        return sq, sk, False, at(sq, sk)

    def first_head(n, _):
        with jax.named_scope("arrive"):
            arrive(n)
        s0, s1 = other(_pick(2 * n, IN)), other(_pick(2 * n + 1, IN))
        attend(0, [(s0, s0, True, at(s0, s0)), (s1, s1, True, at(s1, s1)), pair(s0, s1)])

        def earlier(m, _):
            s2, s3 = other(_pick(2 * m, IN)), other(_pick(2 * m + 1, IN))
            attend(0, [pair(s, t) for t in (s2, s3) for s in (s0, s1)])
            return _

        with jax.named_scope("earlier"):
            lax.fori_loop(0, n, earlier, None)

        @pl.when(n == 1)
        def _():
            with jax.named_scope("pass_on"):
                pass_on(1)

        @pl.when(n == 0)
        def _():
            for h, late in enumerate(LATE, 1):
                for i in late:
                    q_copy(h, i).start()

        return _

    def finish(h, sq, slots, shown=None):
        t = [tops[n] for n in slots]
        if shown is not None:
            t = [jnp.where(show, x, HIDDEN) for show, x in zip(shown, t)]
        top = functools.reduce(jnp.maximum, t)
        acc = sum(part[n] * jnp.exp2((x - top) * E)[:1] for n, x in zip(slots, t))
        o_out[h, sq] = (acc[:HEAD] * (1 / acc[HEAD : HEAD + 1])).T.astype(BF16)

    with jax.named_scope("head_0"):
        lax.fori_loop(0, CHIPS // 2, first_head, None)
    with jax.named_scope("finish"):
        for sq in range(CHIPS):
            finish(0, sq, [at(sq, n) for n in range(sq + 1)])
        for i in range(CHIPS - 1):
            o_copy(0, i).start()

    def later_head(h, _):
        with jax.named_scope("q_wait"):
            received(qs.at[h, pl.ds(0, CHIPS - 1)], q_rs.at[3 + h])

        def two(r, _):
            s0 = other(_pick(2 * r, OUT))
            big, small = jnp.maximum(s0, CHIPS - 1 - s0), jnp.minimum(s0, CHIPS - 1 - s0)
            items = [(big, big, True, 0), (small, small, True, 1)]
            for j in range(CHIPS - 1):
                items.append((jnp.where(j < big, big, small), jnp.where(j < big, j, j - big), False, j + 2))
            for n in range(0, len(items), STEP):
                attend(h, items[n : n + STEP])
            finish(h, big, (0, *range(2, 9)), [True, *(j < big for j in range(CHIPS - 1))])
            finish(h, small, (1, *range(2, 9)), [True, *(j >= big for j in range(CHIPS - 1))])
            o_copy(h, 2 * r).start()

            @pl.when(r < CHIPS // 2 - 1)
            def _():
                o_copy(h, 2 * r + 1).start()

            return _

        with jax.named_scope("rounds"):
            lax.fori_loop(0, CHIPS // 2, two, None)
        return _

    lax.fori_loop(1, GROUP, later_head, None)

    def columns(parts, first, last):
        width = LAST_COLS if last else COLS

        def body(n, _):
            cols = pl.ds(pl.multiple_of(n * width, width), width)
            seen = jnp.concatenate([os[h, g] for h, g in parts], axis=1)
            w = jnp.concatenate([wos[h, pl.ds(pl.multiple_of(g * HEAD, HEAD), HEAD), cols] for h, g in parts], axis=0)
            r = _dot(seen, w, 1, 0)
            r += xs[:, cols].astype(F32) if first else yacc[:, cols]
            if last:
                y_ref[:, cols] = r.astype(BF16)
            else:
                yacc[:, cols] = r
            return _

        with jax.named_scope("columns"):
            lax.fori_loop(0, D // width, body, None)

    own_o = [pltpu.make_async_copy(o_out.at[h, chip], os.at[h, chip], own_sem) for h in range(GROUP)]
    begin(own_o)
    done(os.at[pl.ds(0, GROUP), 0], own_sem)
    with jax.named_scope("wo_wait"):
        done(wos, wo_sem)
    with jax.named_scope("o_wait"):
        received(os.at[0, pl.ds(0, CHIPS - 1)], o_rs.at[0])
    columns([(0, g) for g in range(CHIPS)], True, False)
    with jax.named_scope("o_wait"):
        received(os.at[1, pl.ds(0, CHIPS - 1)], o_rs.at[1])
    columns([(1, g) for g in range(CHIPS)], False, False)
    for n, (p0, p1) in enumerate(zip(PARTS, PARTS[1:])):
        with jax.named_scope("o_wait"):
            received(os.at[2, pl.ds(0, min(p1, CHIPS - 1) - p0)], o_rs.at[2 + n])
        columns([(2, other(m)) for m in OUT[p0:p1]], False, p1 == CHIPS)

    with jax.named_scope("sent"):
        sent(kv.at[pl.ds(0, CHIPS)], rl_ss.at[0])
        sent(kv_out.at[pl.ds(0, CHIPS - 1)], kv_ss.at[0])
        sent(q_out.at[pl.ds(0, GROUP), pl.ds(0, CHIPS - 1)], q_ss.at[0])
        sent(o_out.at[pl.ds(0, GROUP), pl.ds(0, CHIPS - 1)], o_ss.at[0])


def _tables():
    rate = float(THETA) ** (-np.arange(HALF) / HALF)
    def both(place):
        angle = np.tile(place[:, None] * rate, 2)
        return np.stack([np.cos(angle), np.sin(angle)]).astype(np.float32)
    return both(np.arange(ROWS, dtype=np.float64)), both(ROWS * np.arange(2 * CHIPS, dtype=np.float64))


def solution(mesh):
    rot, off = _tables()
    dma = pltpu.SemaphoreType.DMA
    anywhere, vmem = pl.BlockSpec(memory_space=pl.ANY), pl.BlockSpec(memory_space=pltpu.VMEM)

    def step(x, gain, wq, wk, wv, wo):
        block = (ROWS, HEAD)
        return pl.pallas_call(
            _kernel,
            out_shape=pltpu.VMEM((ROWS, D), BF16),
            in_specs=[anywhere] * 8,
            out_specs=vmem,
            scratch_shapes=[
                pltpu.VMEM((ROWS, D), BF16),
                pltpu.VMEM((D,), BF16),
                pltpu.VMEM((2, *block), F32),
                pltpu.VMEM((2, 2 * CHIPS, HEAD), F32),
                pltpu.VMEM((ROWS, D), BF16),
                pltpu.VMEM(block, F32),
                pltpu.VMEM(block, F32),
                pltpu.VMEM((SLOTS, D, 2 * HEAD), BF16),
                pltpu.VMEM((GROUP, CHIPS * HEAD, D), BF16),
                pltpu.VMEM((CHIPS, 2 * ROWS, HEAD), BF16),
                pltpu.VMEM((2 * CHIPS, 2 * ROWS, HEAD), BF16),
                pltpu.VMEM((GROUP, CHIPS, *block), BF16),
                pltpu.VMEM((GROUP, CHIPS, *block), BF16),
                pltpu.VMEM((GROUP, CHIPS, *block), BF16),
                pltpu.VMEM((GROUP, CHIPS, *block), BF16),
                pltpu.VMEM((CHIPS * (CHIPS + 1) // 2, HEAD + 8, ROWS), F32),
                pltpu.VMEM((CHIPS * (CHIPS + 1) // 2, 8, ROWS), F32),
                pltpu.VMEM((ROWS, D), F32),
                dma((X_PARTS,)),
                dma((3,)),
                dma,
                dma((SLOTS,)),
                dma,
                dma((1,)),
                dma((2 + CHIPS // 2,)),
                dma((1,)),
                dma((1,)),
                dma((CHIPS // 2 + GROUP - 1,)),
                dma((1,)),
                dma((GROUP + len(PARTS) - 2,)),
            ],
            compiler_params=pltpu.CompilerParams(collective_id=0, has_side_effects=True, vmem_limit_bytes=62 * 2**20),
        )(x, gain, jnp.asarray(rot), jnp.asarray(off), wq, wk, wv, wo)

    tokens, whole = P(("dp", "sp"), None), P(None, None)
    return jax.shard_map(
        step,
        mesh=mesh,
        in_specs=(tokens, P(None), whole, whole, whole, whole),
        out_specs=tokens,
        check_vma=False,
    )
```
